768 devices in a mesh: dp: 96 (over y, z_lo, core), mp: 8 (over z_hi, x).
Axes of the slice: x: 4, y: 8, z: 12 (z_hi: 2, z_lo: 6; z = z_hi * 6 + z_lo), core: 2. Of those that a mesh axis runs over, the one named last changes fastest.
Arguments:
- hidden_rows: bfloat16 [49152, 3584], P('dp'), may hold values from -6 to 6
- key_grad: bfloat16 [49152, 512], P('dp', 'mp'), may hold values from -6 to 6
- value_grad: bfloat16 [49152, 512], P('dp', 'mp'), may hold values from -6 to 6
- visual_rows: bfloat16 [24576, 1024], P('dp'), may hold values from -6 to 6
- visual_cotangent: bfloat16 [96, 4, 64, 3584], P('dp'), may hold values from -6 to 6
- norm_gain: float32 [1024], replicated, may hold values from 0.25 to 1.75
- norm_bias: float32 [1024], replicated, may hold values from -3 to 3
- fc1_weight: bfloat16 [1024, 4096], P(None, 'mp'), may hold values from -0.1875 to 0.1875
- fc1_bias: float32 [4096], P('mp'), may hold values from -3 to 3
- fc2_weight: bfloat16 [4096, 1024], P('mp'), may hold values from -0.09375 to 0.09375
- fc2_bias: float32 [1024], replicated, may hold values from -3 to 3
- layer_scale: float32 [1024], replicated, may hold values from 0.3 to 1.5
- token_counts: int32 [96, 8], P('dp'), may hold values from 1 to 32, as said below
- dest_offsets: int32 [96, 8], P('dp'), may hold values from 1 to 4, as said below
Outputs:
- key_weight_grad: float32 [3648, 512], P('dp', 'mp')
- value_weight_grad: float32 [3648, 512], P('dp', 'mp')
- projector_grad: float32 [3648, 1024], P('dp', 'mp')
- handoff: bfloat16 [96, 4, 64, 1024], P('dp', None, None, 'mp')
The draws below stay inside these ranges and needn't reach their ends.
Inputs may be any that keep to these rules, and one draw needn't show every extreme that they name: `token_counts`: on every data rank the images of one distance, chosen per rank, all have 32 rows. `dest_offsets`: every data rank sends exactly 2 images to each distance from 1 to 4.
All inputs are finite; a program needn't handle non-finite values.
Results may differ from the reference program's by a relative error of at most 0.0046.
Values may be sent and summed in bfloat16 or wider, within the bound.
A program may use at most 64 MiB of HBM per device.

```python
import math
import jax
import jax.numpy as jnp
from jax import lax

D = 3584
KV_WIDTH = 512
FEAT = 1024
MLP = 4096
TOK_DEV = 512
MOST_TOK = 32
SPREAD = 4
IMG_DEV = 8
ROWS_DEV = 256
CAP = 64
TOKENS = 49152
D_PAD = 3648
N_DP = 96


def routing_table(key):
    base = jax.random.fold_in(key, 11)
    source_keys = jax.random.split(base, N_DP)

    def one_source(source_key):
        first, second, third = jax.random.split(source_key, 3)
        order = jax.random.permutation(first, IMG_DEV)
        offsets = (order % SPREAD + 1).astype(jnp.int32)
        counts = jax.random.randint(second, (IMG_DEV,), 1, MOST_TOK + 1).astype(jnp.int32)
        filled = jax.random.randint(third, (), 1, SPREAD + 1).astype(jnp.int32)
        counts = jnp.where(offsets == filled, MOST_TOK, counts).astype(jnp.int32)
        return (counts, offsets)
    return jax.vmap(one_source)(source_keys)


def draw_token_counts(key, part):
    return routing_table(key)[0]


def draw_dest_offsets(key, part):
    return routing_table(key)[1]


def level_of(key, shape, cuts, low, high):
    factor_of = 1.0
    for dim, shards_of in cuts:
        heights = jax.random.uniform(jax.random.fold_in(jax.random.fold_in(key, 6), dim), (shards_of,), jnp.float32, low / len(cuts), high / len(cuts))
        factor_of = factor_of * jnp.repeat(jnp.exp(heights), shape[dim] // shards_of).reshape((-1,) + (1,) * (len(shape) - 1 - dim))
    return factor_of


def centred(stream_key, extent, spread, most, cuts=(), held_as=jnp.bfloat16):
    factor_of = level_of(stream_key, extent, cuts, -0.22, 0.18) if cuts else 1.0
    array = jax.random.normal(stream_key, extent, jnp.float32) * spread * factor_of
    return jnp.minimum(jnp.maximum(array, -most), most).astype(held_as)


def setup_inputs(seed: int = 0) -> dict:
    keys = jax.random.split(jax.random.key(seed), 15)
    return {
        "hidden_rows": centred(keys[0], (TOKENS, D), 1.0, 6.0, ((0, 96),)),
        "key_grad": centred(keys[1], (TOKENS, KV_WIDTH), 1.0, 6.0, ((0, 96), (1, 8))),
        "value_grad": centred(keys[2], (TOKENS, KV_WIDTH), 1.0, 6.0, ((0, 96), (1, 8))),
        "visual_rows": centred(keys[3], (N_DP * ROWS_DEV, FEAT), 1.0, 6.0, ((0, 96),)),
        "visual_cotangent": centred(keys[4], (N_DP, SPREAD, CAP, D), 1.0, 6.0, ((0, 96),)),
        "norm_gain": jnp.clip(1.0 + 0.15 * jax.random.normal(keys[5], (FEAT,), jnp.float32), 0.25, 1.75),
        "norm_bias": centred(keys[6], (FEAT,), 0.5, 3.0, (), jnp.float32),
        "fc1_weight": centred(keys[7], (FEAT, MLP), FEAT ** -0.5, 0.1875, ((1, 8),)),
        "fc1_bias": centred(keys[8], (MLP,), 0.5, 3.0, ((0, 8),), jnp.float32),
        "fc2_weight": centred(keys[9], (MLP, FEAT), MLP ** -0.5, 0.09375, ((0, 8),)),
        "fc2_bias": centred(keys[10], (FEAT,), 0.5, 3.0, (), jnp.float32),
        "layer_scale": jnp.clip(jnp.exp(jax.random.uniform(keys[11], (FEAT,), jnp.float32, math.log(0.3), math.log(1.5))), 0.3, 1.5),
        "token_counts": draw_token_counts(jax.random.fold_in(keys[14], 71), 0),
        "dest_offsets": draw_dest_offsets(jax.random.fold_in(keys[14], 71), 0),
    }


def pack_rows(rows, counts, offsets):
    total_rows = rows.shape[0]
    images = counts.shape[0]
    counts = counts.astype(jnp.int32)
    offsets = offsets.astype(jnp.int32)
    ends = jnp.cumsum(counts).astype(jnp.int32)
    starts = (ends - counts).astype(jnp.int32)
    places = jnp.arange(total_rows).astype(jnp.int32)
    image_ids = jnp.arange(images).astype(jnp.int32)
    owner = lax.optimization_barrier(jnp.sum((places[:, None] >= ends[None, :]).astype(jnp.int32), axis=1)).astype(jnp.int32)
    member = (owner[:, None] == image_ids[None, :]).astype(jnp.int32)
    earlier = (image_ids[None, :] < image_ids[:, None]) & (offsets[None, :] == offsets[:, None])
    before = lax.optimization_barrier(jnp.sum(earlier.astype(jnp.int32) * counts[None, :], axis=1)).astype(jnp.int32)
    row_dest = lax.optimization_barrier(jnp.sum(member * offsets[None, :], axis=1)).astype(jnp.int32)
    row_start = lax.optimization_barrier(jnp.sum(member * starts[None, :], axis=1)).astype(jnp.int32)
    row_before = lax.optimization_barrier(jnp.sum(member * before[None, :], axis=1)).astype(jnp.int32)
    slot_index = row_before + places - row_start
    target = jnp.where(places < ends[images - 1], (row_dest - 1) * CAP + slot_index, -1).astype(jnp.int32)
    slot_ids = jnp.arange(SPREAD * CAP).astype(jnp.int32)
    select = (slot_ids[:, None] == target[None, :]).astype(jnp.bfloat16)
    packed = jnp.dot(select, rows, preferred_element_type=jnp.float32).astype(jnp.bfloat16)
    return packed.reshape(SPREAD, CAP, rows.shape[1])

def encode(rows, norm_gain, norm_bias, fc1_weight, fc1_bias, fc2_weight, fc2_bias, layer_scale):
    values = rows.astype(jnp.float32)
    center = lax.optimization_barrier(jnp.mean(values, axis=1, keepdims=True))
    spread_sq = lax.optimization_barrier(jnp.mean((values - center) ** 2, axis=1, keepdims=True))
    normed = ((values - center) * lax.rsqrt(spread_sq + 1e-06) * norm_gain + norm_bias).astype(jnp.bfloat16)
    hidden = jax.nn.gelu(jnp.dot(normed, fc1_weight, preferred_element_type=jnp.float32) + fc1_bias, approximate=False).astype(jnp.bfloat16)
    partial_value = jnp.dot(hidden, fc2_weight, preferred_element_type=jnp.float32)
    return (values + layer_scale * (partial_value + fc2_bias)).astype(jnp.bfloat16)

def reference(hidden_rows, key_grad, value_grad, visual_rows, visual_cotangent, norm_gain, norm_bias, fc1_weight, fc1_bias, fc2_weight, fc2_bias, layer_scale, token_counts, dest_offsets):
    width = hidden_rows.shape[1]
    blocks = hidden_rows.reshape(N_DP, TOK_DEV, width)
    key_blocks = key_grad.reshape(N_DP, TOK_DEV, KV_WIDTH)
    value_blocks = value_grad.reshape(N_DP, TOK_DEV, KV_WIDTH)

    def accumulate(carry, pieces):
        inputs, key_piece, value_piece = pieces
        key_total, value_total = carry
        key_total = key_total + lax.dot_general(inputs, key_piece, (((0,), (0,)), ((), ())), preferred_element_type=jnp.float32)
        value_total = value_total + lax.dot_general(inputs, value_piece, (((0,), (0,)), ((), ())), preferred_element_type=jnp.float32)
        return ((key_total, value_total), None)
    empty = jnp.zeros((width, KV_WIDTH), jnp.float32)
    (key_total, value_total), _ = lax.scan(accumulate, (empty, empty), (blocks, key_blocks, value_blocks))
    key_bias = lax.optimization_barrier(jnp.sum(key_grad.astype(jnp.float32), axis=0))[None, :]
    value_bias = lax.optimization_barrier(jnp.sum(value_grad.astype(jnp.float32), axis=0))[None, :]
    zero_rows = jnp.zeros((D_PAD - width - 1, KV_WIDTH), jnp.float32)
    key_weight_grad = jnp.concatenate([key_total, key_bias, zero_rows], axis=0)
    value_weight_grad = jnp.concatenate([value_total, value_bias, zero_rows], axis=0)
    encoded = encode(visual_rows, norm_gain, norm_bias, fc1_weight, fc1_bias, fc2_weight, fc2_bias, layer_scale)
    packed = jax.vmap(pack_rows)(encoded.reshape(N_DP, ROWS_DEV, FEAT), token_counts, dest_offsets)
    handoff = jnp.stack([jnp.roll(packed[:, distance], distance + 1, axis=0) for distance in range(SPREAD)], axis=1)
    cot_flat = visual_cotangent.reshape(N_DP * SPREAD * CAP, width)
    rows_flat = handoff.reshape(N_DP * SPREAD * CAP, FEAT)
    projector_main = lax.dot_general(cot_flat, rows_flat, (((0,), (0,)), ((), ())), preferred_element_type=jnp.float32)
    projector_grad = jnp.concatenate([projector_main, jnp.zeros((D_PAD - width, FEAT), jnp.float32)], axis=0)
    return (key_weight_grad, value_weight_grad, projector_grad, handoff)
```

```python
import functools

import jax
import jax.numpy as jnp
from jax import lax
from jax.experimental import pallas as pl
from jax.experimental.pallas import tpu as pltpu
from jax.sharding import PartitionSpec as P

MESH = pl.DeviceIdType.MESH
F32 = jnp.float32
BF16 = jnp.bfloat16

NX, NY, NZ, NCORE, NHALF = 4, 8, 6, 2, 2
N_DP = NY * NZ * NCORE
SPREAD, CAP = 4, 64
SLOTS = SPREAD * CAP
IMAGES = 8
OWN = 38
BLK = 40
YROWS = NZ * NCORE * OWN


def kernel(
    hid_hbm, kg_hbm, vg_hbm, vis_hbm, cot_hbm, gain_hbm, nb_hbm, w1_hbm, b1_hbm, w2_hbm, b2_hbm, ls_hbm,
    cnt_ref, off_ref,
    key_o, val_o, proj_o, hand_o,
    hid, kg, vg, vis, cot, gain, nb, w1, b1, w2, b2, ls,
    packed, part, xs, xr, vs, vr, hs, hr, hand, hpar,
    kvf, kvo, kvp, cotf, amat, apar,
    s1, r1y, r1z, s2, r2, keyv, valv, projv,
    lsem, osem, dsem_s, dsem_r, xsem_s, xsem_r, vsem_s, vsem_r, hsem_s, hsem_r,
    y_s, y_r, z_s, z_r,
):
    dp = lax.axis_index("dp")
    mp = lax.axis_index("mp")
    core = lax.rem(dp, 2)
    zlo = lax.rem(lax.div(dp, 2), NZ)
    y = lax.div(dp, NZ * NCORE)
    zhi = lax.div(mp, NX)
    x = lax.rem(mp, NX)
    partner = (dp + 1 - 2 * core, mp)

    def rank_of(y_, z_):
        return (y_ * NZ + z_) * NCORE + core

    loads = [
        (vis_hbm, vis), (w1_hbm, w1), (gain_hbm, gain), (nb_hbm, nb), (b1_hbm, b1), (w2_hbm, w2),
        (b2_hbm, b2), (ls_hbm, ls), (kg_hbm, kg), (vg_hbm, vg), (hid_hbm, hid), (cot_hbm.at[0], cot),
    ]
    copies = [pltpu.make_async_copy(s, d, lsem.at[i]) for i, (s, d) in enumerate(loads)]
    for c in copies:
        c.start()
    (l_vis, l_w1, l_gain, l_nb, l_b1, l_w2, l_b2, l_ls, l_kg, l_vg, l_hid, l_cot) = copies

    barrier = pltpu.get_barrier_semaphore()
    greeted = [partner]
    greeted += [(rank_of(lax.rem(y + d, NY), zlo), mp) for d in range(1, NY)]
    greeted += [(rank_of(y, lax.rem(zlo + d, NZ)), mp) for d in range(1, NZ)]
    greeted += [(dp, zhi * NX + lax.rem(x + d, NX)) for d in range(1, NX)]
    for k in range(1, SPREAD + 1):
        for e in range(NHALF):
            greeted.append((lax.rem(dp + k, N_DP), e * NX + x))
            greeted.append((lax.rem(dp + N_DP - k, N_DP), e * NX + x))
    for who in greeted:
        pl.semaphore_signal(barrier, 1, device_id=who, device_id_type=MESH)

    place = lax.broadcasted_iota(jnp.int32, (1, SLOTS), 1)
    target = jnp.full((1, SLOTS), -1, jnp.int32)
    counts = [cnt_ref[0, i] for i in range(IMAGES)]
    offs = [off_ref[0, i] for i in range(IMAGES)]
    start = jnp.int32(0)
    for i in range(IMAGES):
        end = start + counts[i]
        before = jnp.int32(0)
        for j in range(i):
            before = before + jnp.where(offs[j] == offs[i], counts[j], 0)
        base = (offs[i] - 1) * CAP + before - start
        inside = (place >= start) & (place < end)
        target = jnp.where(inside, place + base, target)
        start = end
    filled = []
    for k in range(1, SPREAD + 1):
        total = jnp.int32(0)
        for i in range(IMAGES):
            total = total + jnp.where(offs[i] == k, counts[i], 0)
        filled.append(total)
    slot_ids = lax.broadcasted_iota(jnp.int32, (SLOTS, SLOTS), 0)
    select = jnp.where(slot_ids == target, 1.0, 0.0).astype(BF16)

    l_vis.wait()
    packed[...] = jnp.dot(select, vis[...], preferred_element_type=F32).astype(BF16)
    values = packed[...].astype(F32)
    center = jnp.mean(values, axis=1, keepdims=True)
    delta = values - center
    spread_sq = jnp.mean(delta * delta, axis=1, keepdims=True)
    l_gain.wait()
    l_nb.wait()
    normed = (delta * lax.rsqrt(spread_sq + 1e-06) * gain[...] + nb[...]).astype(BF16)
    l_w1.wait()
    l_b1.wait()
    pre = jnp.dot(normed, w1[...], preferred_element_type=F32) + b1[...]
    hidden = (0.5 * pre * (1.0 + lax.erf(pre * (0.5**0.5)))).astype(BF16)
    l_w2.wait()
    part[...] = jnp.dot(hidden, w2[...], preferred_element_type=F32)
    for xd in range(NX):
        for e in range(NHALF):
            cols = (e * NX + xd) * 128
            for k in range(SPREAD):
                xs[xd, k, e] = part[k * CAP : (k + 1) * CAP, cols : cols + 128].astype(BF16)

    pl.semaphore_wait(barrier, len(greeted))

    def x_copy(d, k):
        return pltpu.make_async_remote_copy(
            src_ref=xs.at[lax.rem(x + d, NX), k], dst_ref=xr.at[d - 1, k],
            send_sem=xsem_s.at[d - 1, k], recv_sem=xsem_r.at[d - 1, k],
            device_id=(dp, zhi * NX + lax.rem(x + d, NX)), device_id_type=MESH,
        )

    for k in range(SPREAD):
        for d in (2, 1, 3):
            x_copy(d, k).start()

    def v_copy(k):
        return pltpu.make_async_remote_copy(
            src_ref=vs.at[k], dst_ref=vr.at[k], send_sem=vsem_s.at[k], recv_sem=vsem_r.at[k],
            device_id=(lax.rem(dp + k + 1, N_DP), mp), device_id_type=MESH,
        )

    own_cols = pl.ds(pl.multiple_of(mp * 128, 128), 128)
    for k in range(SPREAD):
        vs[k] = packed[k * CAP : (k + 1) * CAP, own_cols]
        v_copy(k).start()

    l_kg.wait()
    l_vg.wait()
    l_hid.wait()
    kv = jnp.concatenate([kg[...], vg[...]], axis=1)

    @pl.loop(0, 7)
    def _(i):
        cols = pl.ds(pl.multiple_of(i * 512, 512), 512)
        kvf[cols, :] = lax.dot_general(
            hid[:, cols], kv, (((0,), (0,)), ((), ())), preferred_element_type=F32
        )

    colsum = jnp.sum(kv.astype(F32), axis=0, keepdims=True)
    tail_row = lax.broadcasted_iota(jnp.int32, (80, 128), 0)
    kvf[3584:3664, :] = jnp.where(tail_row == 0, colsum, 0.0)

    @pl.loop(0, NY)
    def _(yy):
        win = kvf[pl.ds(pl.multiple_of(yy * YROWS, 8), YROWS + 8), :]
        for z in range(NZ):
            for c in range(NCORE):
                at = (z * NCORE + c) * OWN
                kvo[c, yy, z] = win[at : at + BLK, :]

    def d_copy(src, dst, i):
        return pltpu.make_async_remote_copy(
            src_ref=src, dst_ref=dst, send_sem=dsem_s.at[i], recv_sem=dsem_r.at[i],
            device_id=partner, device_id_type=MESH,
        )

    kv_swap = d_copy(kvo.at[1 - core], kvp, 0)
    kv_swap.start()

    def y_copy(g, d):
        to = lax.rem(y + d, NY)
        return pltpu.make_async_remote_copy(
            src_ref=s1.at[g, to], dst_ref=r1y.at[g, d - 1],
            send_sem=y_s.at[g, d - 1], recv_sem=y_r.at[g, d - 1],
            device_id=(rank_of(to, zlo), mp), device_id_type=MESH,
        )

    def z_copy(g, d):
        to = lax.rem(zlo + d, NZ)
        return pltpu.make_async_remote_copy(
            src_ref=s2.at[g, to], dst_ref=r2.at[g, d - 1],
            send_sem=z_s.at[g, d - 1], recv_sem=z_r.at[g, d - 1],
            device_id=(rank_of(y, to), mp), device_id_type=MESH,
        )

    kv_swap.wait()

    @pl.loop(0, NY)
    def _(yy):
        s1[0, yy] = (kvo[core, yy] + kvp[yy]).astype(BF16)

    for d in (4, 3, 5, 2, 6, 1, 7):
        y_copy(0, d).start()

    def h_copy(e, k):
        return pltpu.make_async_remote_copy(
            src_ref=hs.at[e, k], dst_ref=hr.at[zhi, k], send_sem=hsem_s.at[e, k], recv_sem=hsem_r.at[zhi, k],
            device_id=(lax.rem(dp + k + 1, N_DP), e * NX + x), device_id_type=MESH,
        )

    def h_wait(e, k):
        pltpu.make_async_remote_copy(
            src_ref=hs.at[e, k], dst_ref=hr.at[e, k], send_sem=hsem_s.at[e, k], recv_sem=hsem_r.at[e, k],
            device_id=(lax.rem(dp + k + 1, N_DP), e * NX + x), device_id_type=MESH,
        ).wait_recv()

    l_b2.wait()
    l_ls.wait()
    with_bias = jnp.where(zhi == 0, 1.0, 0.0)
    slot_in = lax.broadcasted_iota(jnp.int32, (CAP, 128), 0)
    for k in range(SPREAD):
        for d in range(1, NX):
            x_copy(d, k).wait_recv()
        for e in range(NHALF):
            cols = pl.ds(pl.multiple_of((e * NX + x) * 128, 128), 128)
            total = part[k * CAP : (k + 1) * CAP, cols]
            for d in range(1, NX):
                total = total + xr[d - 1, k, e].astype(F32)
            branch = ls[:, cols] * (total + with_bias * b2[:, cols])
            hs[e, k] = jnp.where(slot_in < filled[k], branch, 0.0).astype(BF16)
            h_copy(e, k).start()

    l_cot.wait()

    @pl.loop(0, 28)
    def _(i):
        cols = pl.ds(pl.multiple_of(i * 128, 128), 128)
        block = cot[:, :, cols].reshape(SLOTS, 128).astype(F32)
        cotf[cols, :] = block.T

    cotf[3584:3664, :] = jnp.zeros((80, SLOTS), F32)

    @pl.loop(0, NY)
    def _(yy):
        win = cotf[pl.ds(pl.multiple_of(yy * YROWS, 8), YROWS + 8), :]
        for c in range(NCORE):
            rows = [win[(z * NCORE + c) * OWN : (z * NCORE + c) * OWN + BLK, :] for z in range(NZ)]
            amat[c, yy] = jnp.concatenate(rows, axis=0).astype(BF16)

    a_swap = d_copy(amat.at[1 - core], apar, 1)
    a_swap.start()

    for k in range(SPREAD):
        v_copy(k).wait_recv()
        for e in range(NHALF):
            h_wait(e, k)
        hand[k] = (vr[k].astype(F32) + (hr[0, k].astype(F32) + hr[1, k].astype(F32))).astype(BF16)
    h_swap = d_copy(hand, hpar, 2)
    h_swap.start()
    out_hand = pltpu.make_async_copy(hand, hand_o.at[0], osem.at[0])
    out_hand.start()
    a_swap.wait()
    h_swap.wait()
    mine = hand[...].reshape(SLOTS, 128)
    theirs = hpar[...].reshape(SLOTS, 128)

    @pl.loop(0, NY)
    def _(yy):
        res = jnp.dot(amat[core, yy], mine, preferred_element_type=F32)
        res = res + jnp.dot(apar[yy], theirs, preferred_element_type=F32)
        for z in range(NZ):
            s1[1, yy, z] = res[z * BLK : (z + 1) * BLK, :].astype(BF16)

    for d in (4, 3, 5, 2, 6, 1, 7):
        y_copy(1, d).start()

    for g in range(2):
        total = s1[g, y].astype(F32)
        for d in range(1, NY):
            y_copy(g, d).wait_recv()
            total = total + r1y[g, d - 1].astype(F32)
        s2[g] = total.astype(BF16)
        for d in (5, 4, 3, 2, 1):
            z_copy(g, d).start()
    for g in range(2):
        total = s2[g, zlo].astype(F32)
        for d in range(1, NZ):
            z_copy(g, d).wait_recv()
            total = total + r2[g, d - 1].astype(F32)
        if g == 0:
            keyv[...] = total[:OWN, :64]
            valv[...] = total[:OWN, 64:]
            out_key = pltpu.make_async_copy(keyv, key_o, osem.at[1])
            out_val = pltpu.make_async_copy(valv, val_o, osem.at[2])
            out_key.start()
            out_val.start()
        else:
            projv[...] = total[:OWN, :]
            out_proj = pltpu.make_async_copy(projv, proj_o, osem.at[3])
            out_proj.start()

    for k in range(SPREAD):
        for d in range(1, NX):
            x_copy(d, k).wait_send()
        v_copy(k).wait_send()
        for e in range(NHALF):
            h_copy(e, k).wait_send()
    for g in range(2):
        for d in range(1, NY):
            y_copy(g, d).wait_send()
        for d in range(1, NZ):
            z_copy(g, d).wait_send()
    out_hand.wait()
    out_key.wait()
    out_val.wait()
    out_proj.wait()


def per_device(
    hidden_rows, key_grad, value_grad, visual_rows, visual_cotangent, norm_gain, norm_bias,
    fc1_weight, fc1_bias, fc2_weight, fc2_bias, layer_scale, token_counts, dest_offsets,
):
    anyspec = pl.BlockSpec(memory_space=pl.ANY)
    smem = pl.BlockSpec(memory_space=pltpu.SMEM)
    dma = pltpu.SemaphoreType.DMA
    V = pltpu.VMEM
    scratch = [
        V((512, 3584), BF16), V((512, 64), BF16), V((512, 64), BF16), V((256, 1024), BF16),
        V((4, 64, 3584), BF16), V((1, 1024), F32), V((1, 1024), F32), V((1024, 512), BF16), V((1, 512), F32),
        V((512, 1024), BF16), V((1, 1024), F32), V((1, 1024), F32),
        V((256, 1024), BF16), V((256, 1024), F32),
        V((NX, SPREAD, NHALF, CAP, 128), BF16), V((NX - 1, SPREAD, NHALF, CAP, 128), BF16),
        V((SPREAD, CAP, 128), BF16), V((SPREAD, CAP, 128), BF16),
        V((NHALF, SPREAD, CAP, 128), BF16), V((NHALF, SPREAD, CAP, 128), BF16),
        V((SPREAD, CAP, 128), BF16), V((SPREAD, CAP, 128), BF16),
        V((3664, 128), F32), V((NCORE, NY, NZ, BLK, 128), F32), V((NY, NZ, BLK, 128), F32),
        V((3664, 256), F32), V((NCORE, NY, NZ * BLK, 256), BF16), V((NY, NZ * BLK, 256), BF16),
        V((2, NY, NZ, BLK, 128), BF16), V((2, NY - 1, NZ, BLK, 128), BF16), V((8, 128), F32),
        V((2, NZ, BLK, 128), BF16), V((2, NZ - 1, BLK, 128), BF16),
        V((OWN, 64), F32), V((OWN, 64), F32), V((OWN, 128), F32),
        dma((12,)), dma((4,)), dma((3,)), dma((3,)),
        dma((NX - 1, SPREAD)), dma((NX - 1, SPREAD)), dma((SPREAD,)), dma((SPREAD,)),
        dma((NHALF, SPREAD)), dma((NHALF, SPREAD)),
        dma((2, NY - 1)), dma((2, NY - 1)), dma((2, NZ - 1)), dma((2, NZ - 1)),
    ]
    key_g, value_g, proj_g, handoff = pl.pallas_call(
        kernel,
        out_shape=(
            jax.ShapeDtypeStruct((OWN, 64), F32),
            jax.ShapeDtypeStruct((OWN, 64), F32),
            jax.ShapeDtypeStruct((OWN, 128), F32),
            jax.ShapeDtypeStruct((1, SPREAD, CAP, 128), BF16),
        ),
        in_specs=[anyspec] * 12 + [smem] * 2,
        out_specs=[anyspec] * 4,
        scratch_shapes=scratch,
        compiler_params=pltpu.CompilerParams(
            collective_id=0, has_side_effects=True, vmem_limit_bytes=60 * 1024 * 1024
        ),
        name="bucket",
    )(
        hidden_rows, key_grad, value_grad, visual_rows, visual_cotangent,
        norm_gain.reshape(1, -1), norm_bias.reshape(1, -1), fc1_weight, fc1_bias.reshape(1, -1),
        fc2_weight, fc2_bias.reshape(1, -1), layer_scale.reshape(1, -1), token_counts, dest_offsets,
    )
    return key_g, value_g, proj_g, handoff


def solution(mesh):
    placed = (
        P("dp", None), P("dp", "mp"), P("dp", "mp"), P("dp", None), P("dp", None, None, None),
        P(), P(), P(None, "mp"), P("mp"), P("mp", None), P(), P(), P("dp", None), P("dp", None),
    )
    return jax.shard_map(
        per_device,
        mesh=mesh,
        in_specs=placed,
        out_specs=(P("dp", "mp"), P("dp", "mp"), P("dp", "mp"), P("dp", None, None, "mp")),
        check_vma=False,
    )
```

```python
import jax
import jax.numpy as jnp
from jax import lax
from jax.experimental import pallas as pl
from jax.experimental.pallas import tpu as pltpu
from jax.sharding import PartitionSpec as P

MESH = pl.DeviceIdType.MESH
F32 = jnp.float32
BF16 = jnp.bfloat16

NX, NY, NZ, NCORE, NHALF = 4, 8, 6, 2, 2
N_DP = NY * NZ * NCORE
N_CHIP = NY * NZ
SPREAD, CAP = 4, 64
SLOTS = SPREAD * CAP
IMAGES = 8
OWN = 38
BLK = 40
YROWS = NZ * NCORE * OWN
WIDE = 3584
FAR_Y = (4, 3, 5, 2, 6, 1, 7)
FAR_Z = ((5, 4, 3, 2, 1), (5, 4, 3, 0, 2), (5, 4, 0, 3, 1), (0, 1, 5, 2, 4), (0, 1, 2, 5, 3), (0, 1, 2, 3, 4))


def kernel(
    hid_hbm, kgt_hbm, vgt_hbm, vis_hbm, cot_hbm, gain_hbm, nb_hbm, w1_hbm, b1_hbm, w2_hbm, b2_hbm, ls_hbm,
    cnt_hbm, off_hbm,
    keyv, valv, projv, hand,
    hid, kvt, vis, cot, gain, nb, w1, b1, w2, b2, ls, cnt, off,
    packed, part, xs, xr, vs, vr, hs, hr, hpar,
    kvf, kvo, kvp, cotf, amat, apar, half,
    s1k, r1k, s2k, r2k, s1p, r1a, r1b, s2a, s2b, r2a, r2b,
    lsem, dsem_s, dsem_r, hpsem_s, hpsem_r, xsem_s, xsem_r, vsem_s, vsem_r, hsem_s, hsem_r,
    ky_s, ky_r, kz_s, kz_r, p1_s, p1_r, p2_s, p2_r, go,
):
    dp = lax.axis_index("dp")
    mp = lax.axis_index("mp")
    core = lax.rem(dp, NCORE)
    chip = lax.div(dp, NCORE)
    zlo = lax.rem(chip, NZ)
    y = lax.div(chip, NZ)
    zhi = lax.div(mp, NX)
    x = lax.rem(mp, NX)
    partner = (dp + 1 - 2 * core, mp)

    def rank_of(y_, z_):
        return (y_ * NZ + z_) * NCORE + core

    def far_z(i):
        to = jnp.int32(0)
        for q in range(NZ):
            to = jnp.where(zlo == q, FAR_Z[q][i], to)
        return to

    far = [far_z(i) for i in range(NZ - 1)]
    others = [lax.rem(zlo + d, NZ) for d in range(1, NZ)]

    def remote(src, dst, send, recv, who):
        return pltpu.make_async_remote_copy(
            src_ref=src, dst_ref=dst, send_sem=send, recv_sem=recv, device_id=who, device_id_type=MESH
        )

    loads = [
        (cnt_hbm, cnt), (off_hbm, off), (vis_hbm, vis), (gain_hbm, gain), (nb_hbm, nb), (w1_hbm, w1),
        (b1_hbm, b1), (w2_hbm, w2), (b2_hbm, b2), (ls_hbm, ls), (kgt_hbm, kvt.at[0:64]),
        (vgt_hbm, kvt.at[64:128]), (hid_hbm, hid), (cot_hbm.at[0], cot),
    ]
    copies = [pltpu.make_async_copy(s, d, lsem.at[i]) for i, (s, d) in enumerate(loads)]
    for c in copies[:12]:
        c.start()
    (l_cnt, l_off, l_vis, l_gain, l_nb, l_w1, l_b1, l_w2, l_b2, l_ls, l_kg, l_vg, l_hid, l_cot) = copies

    barrier = pltpu.get_barrier_semaphore()

    def greet(dp_, mp_):
        pl.semaphore_signal(barrier, 1, device_id=(dp_, mp_), device_id_type=MESH)

    for d in range(1, NX):
        greet(chip * NCORE, zhi * NX + lax.rem(x + d, NX))

    @pl.when(core == 1)
    def _():
        greet(chip * NCORE, mp)

    for d in range(1, NY):
        greet((lax.rem(y + d, NY) * NZ + zlo) * NCORE + 1, mp)
    for d in range(1, NZ):
        greet((y * NZ + lax.rem(zlo + d, NZ)) * NCORE + 1, mp)
    other = (1 - zhi) * NX + x
    for d in (0, 1, 2, N_CHIP - 1, N_CHIP - 2):
        there = lax.rem(chip + d, N_CHIP) * NCORE + 1
        if d:
            greet(there, mp)
        greet(there, other)
    near_count = 2 * (NX - 1) + 1
    far_count = 2 * (NY - 1 + NZ - 1 + 9)

    l_cnt.wait()
    l_off.wait()
    place = lax.broadcasted_iota(jnp.int32, (1, SLOTS), 1)
    target = jnp.full((1, SLOTS), -1, jnp.int32)
    counts = [cnt[0, i] for i in range(IMAGES)]
    offs = [off[0, i] for i in range(IMAGES)]
    start = jnp.int32(0)
    for i in range(IMAGES):
        end = start + counts[i]
        before = jnp.int32(0)
        for j in range(i):
            before = before + jnp.where(offs[j] == offs[i], counts[j], 0)
        base = (offs[i] - 1) * CAP + before - start
        inside = (place >= start) & (place < end)
        target = jnp.where(inside, place + base, target)
        start = end
    filled = []
    for k in range(1, SPREAD + 1):
        total = jnp.int32(0)
        for i in range(IMAGES):
            total = total + jnp.where(offs[i] == k, counts[i], 0)
        filled.append(total)
    slot_ids = lax.broadcasted_iota(jnp.int32, (SLOTS, SLOTS), 0)
    select = jnp.where(slot_ids == target, 1.0, 0.0).astype(BF16)

    l_vis.wait()
    packed[...] = jnp.dot(select, vis[...], preferred_element_type=F32).astype(BF16)
    values = packed[...].astype(F32)
    center = jnp.mean(values, axis=1, keepdims=True)
    delta = values - center
    spread_sq = jnp.mean(delta * delta, axis=1, keepdims=True)
    l_gain.wait()
    l_nb.wait()
    normed = (delta * lax.rsqrt(spread_sq + 1e-06) * gain[...] + nb[...]).astype(BF16)
    l_w1.wait()
    l_b1.wait()
    l_hid.start()
    pre = jnp.dot(normed, w1[...], preferred_element_type=F32) + b1[...]
    hidden = (0.5 * pre * (1.0 + lax.erf(pre * (0.5**0.5)))).astype(BF16)
    l_w2.wait()
    l_cot.start()

    def second(e):
        cols = pl.ds(pl.multiple_of(e * NX * 128, 128), NX * 128)
        res = jnp.dot(hidden, w2[:, cols], preferred_element_type=F32)
        part[e] = res
        for xd in range(NX):
            xs[e, xd] = res[:, xd * 128 : (xd + 1) * 128].astype(BF16).reshape(SPREAD, CAP, 128)

    second(1 - zhi)

    @pl.when(core == 0)
    def _():
        pl.semaphore_wait(barrier, near_count)
        pl.semaphore_signal(go.at[0], 1, device_id=partner, device_id_type=MESH)

    @pl.when(core == 1)
    def _():
        pl.semaphore_wait(go.at[0], 1)

    def x_copy(e, d, k):
        to = lax.rem(x + d, NX)
        return remote(
            xs.at[e, to, k], xr.at[e, d - 1, k], xsem_s.at[e, d - 1, k], xsem_r.at[e, d - 1, k],
            (dp, zhi * NX + to),
        )

    for k in range(SPREAD):
        for d in (2, 1, 3):
            x_copy(1 - zhi, d, k).start()
    second(zhi)
    for k in range(SPREAD):
        for d in (2, 1, 3):
            x_copy(zhi, d, k).start()

    own_cols = pl.ds(pl.multiple_of(mp * 128, 128), 128)
    for k in range(SPREAD):
        vs[k] = packed[k * CAP : (k + 1) * CAP, own_cols]

    l_kg.wait()
    l_vg.wait()
    l_hid.wait()
    kv = kvt[...].astype(F32).T.astype(BF16)

    @pl.loop(0, 7)
    def _(i):
        cols = pl.ds(pl.multiple_of(i * 512, 512), 512)
        kvf[cols, :] = lax.dot_general(
            hid[:, cols], kv, (((0,), (0,)), ((), ())), preferred_element_type=F32
        )

    colsum = jnp.sum(kv.astype(F32), axis=0, keepdims=True)
    tail_row = lax.broadcasted_iota(jnp.int32, (80, 128), 0)
    kvf[WIDE : WIDE + 80, :] = jnp.where(tail_row == 0, colsum, 0.0)

    @pl.loop(0, NY)
    def _(yy):
        win = kvf[pl.ds(pl.multiple_of(yy * YROWS, 8), YROWS + 8), :]
        for z in range(NZ):
            for c in range(NCORE):
                at = (z * NCORE + c) * OWN
                kvo[c, yy, z] = win[at : at + BLK, :]

    kv_swap = remote(kvo.at[1 - core], kvp, dsem_s.at[0], dsem_r.at[0], partner)
    kv_swap.start()

    def v_copy(k):
        return remote(vs.at[k], vr.at[k], vsem_s.at[k], vsem_r.at[k], (lax.rem(dp + k + 1, N_DP), mp))

    def h_copy(e, k):
        to = (lax.rem(dp + k + 1, N_DP), e * NX + x)
        return remote(hs.at[e, k], hr.at[zhi, k], hsem_s.at[e, k], hsem_r.at[zhi, k], to)

    def h_wait(e, k):
        to = (lax.rem(dp + k + 1, N_DP), e * NX + x)
        remote(hs.at[e, k], hr.at[e, k], hsem_s.at[e, k], hsem_r.at[e, k], to).wait_recv()

    l_b2.wait()
    l_ls.wait()
    with_bias = jnp.where(zhi == 0, 1.0, 0.0)
    slot_in = lax.broadcasted_iota(jnp.int32, (CAP, 128), 0)
    @pl.when(core == 1)
    def _():
        pl.semaphore_wait(barrier, far_count)
        pl.semaphore_signal(go.at[1], 1, device_id=partner, device_id_type=MESH)

    @pl.when(core == 0)
    def _():
        pl.semaphore_wait(go.at[1], 1)

    for k in range(SPREAD):
        v_copy(k).start()

    def sum_x(e):
        cols = pl.ds(pl.multiple_of((e * NX + x) * 128, 128), 128)
        own = pl.ds(pl.multiple_of(x * 128, 128), 128)
        for k in range(SPREAD):
            for d in range(1, NX):
                x_copy(e, d, k).wait_recv()
            total = part[e, k * CAP : (k + 1) * CAP, own]
            for d in range(1, NX):
                total = total + xr[e, d - 1, k].astype(F32)
            branch = ls[:, cols] * (total + with_bias * b2[:, cols])
            hs[e, k] = jnp.where(slot_in < filled[k], branch, 0.0).astype(BF16)
            h_copy(e, k).start()

    sum_x(1 - zhi)
    sum_x(zhi)

    def ky_copy(d):
        to = lax.rem(y + d, NY)
        return remote(s1k.at[to], r1k.at[d - 1], ky_s.at[d - 1], ky_r.at[d - 1], (rank_of(to, zlo), mp))

    def kz_copy(to):
        return remote(s2k.at[to], r2k.at[zlo], kz_s.at[to], kz_r.at[zlo], (rank_of(y, to), mp))

    def kz_wait(q):
        remote(s2k.at[q], r2k.at[q], kz_s.at[q], kz_r.at[q], (rank_of(y, q), mp)).wait_recv()

    kv_swap.wait()

    @pl.loop(0, NY)
    def _(yy):
        s1k[yy] = (kvo[core, yy] + kvp[yy]).astype(BF16)

    for d in FAR_Y:
        ky_copy(d).start()

    l_cot.wait()

    @pl.loop(0, 28)
    def _(i):
        cols = pl.ds(pl.multiple_of(i * 128, 128), 128)
        block = cot[:, :, cols].reshape(SLOTS, 128).astype(F32)
        cotf[cols, :] = block.T

    cotf[WIDE : WIDE + 80, :] = jnp.zeros((80, SLOTS), F32)

    @pl.loop(0, NY // 2)
    def _(j):
        win = cotf[pl.ds(pl.multiple_of(j * 2 * YROWS, 8), 2 * YROWS + 8), :]

        def block(yy, z, c):
            at = yy * YROWS + (z * NCORE + c) * OWN
            return win[at : at + BLK, :]

        for yy in range(2):
            rows = jnp.concatenate([block(yy, z, 0) for z in range(NZ)], axis=0).astype(BF16)
            amat[0, pl.ds(pl.multiple_of((2 * j + yy) * NZ * BLK, 16), NZ * BLK), :] = rows
        for z in range(NZ):
            rows = jnp.concatenate([block(0, z, 1), block(1, z, 1)], axis=0).astype(BF16)
            amat[1, pl.ds(pl.multiple_of((z * NY + 2 * j) * BLK, 16), 2 * BLK), :] = rows

    a_swap = remote(amat.at[1 - core], apar, dsem_s.at[1], dsem_r.at[1], partner)
    a_swap.start()

    def hp_copy(k):
        return remote(hand.at[0, k], hpar.at[k], hpsem_s.at[k], hpsem_r.at[k], partner)

    for k in range(SPREAD):
        v_copy(k).wait_recv()
        for e in range(NHALF):
            h_wait(e, k)
        hand[0, k] = (vr[k].astype(F32) + (hr[0, k].astype(F32) + hr[1, k].astype(F32))).astype(BF16)
        hp_copy(k).start()

    half[...] = jnp.dot(amat[core], hand[0].reshape(SLOTS, 128), preferred_element_type=F32)

    a_swap.wait_recv()
    for k in range(SPREAD):
        hp_copy(k).wait_recv()

    theirs = hpar[...].reshape(SLOTS, 128)

    def p1y_copy(d):
        to = lax.rem(y + d, NY)
        return remote(
            s1p.at[pl.ds(to * NZ, NZ)], r1a.at[d - 1], p1_s.at[d - 1], p1_r.at[d - 1], (rank_of(to, zlo), mp)
        )

    def p1z_copy(to):
        return remote(s1p.at[pl.ds(to * NY, NY)], r1b.at[zlo], p1_s.at[to], p1_r.at[zlo], (rank_of(y, to), mp))

    def p1z_wait(q):
        remote(s1p.at[pl.ds(q * NY, NY)], r1b.at[q], p1_s.at[q], p1_r.at[q], (rank_of(y, q), mp)).wait_recv()

    def p2z_copy(to):
        return remote(s2a.at[to], r2a.at[zlo], p2_s.at[to], p2_r.at[zlo], (rank_of(y, to), mp))

    def p2z_wait(q):
        remote(s2a.at[q], r2a.at[q], p2_s.at[q], p2_r.at[q], (rank_of(y, q), mp)).wait_recv()

    def p2y_copy(d):
        to = lax.rem(y + d, NY)
        return remote(s2b.at[to], r2b.at[d - 1], p2_s.at[d - 1], p2_r.at[d - 1], (rank_of(to, zlo), mp))

    def block_rows(to, count):
        rows = pl.ds(pl.multiple_of(to * count * BLK, 16), count * BLK)
        res = half[rows, :] + jnp.dot(apar[rows, :], theirs, preferred_element_type=F32)
        for i in range(count):
            s1p[to * count + i] = res[i * BLK : (i + 1) * BLK, :].astype(BF16)

    @pl.when(core == 0)
    def _():
        for d in FAR_Y:
            block_rows(lax.rem(y + d, NY), NZ)
            p1y_copy(d).start()
        block_rows(y, NZ)

    @pl.when(core == 1)
    def _():
        for to in far:
            block_rows(to, NY)
            p1z_copy(to).start()
        block_rows(zlo, NY)

    total = s1k[y].astype(F32)
    for d in FAR_Y[::-1]:
        ky_copy(d).wait_recv()
        total = total + r1k[d - 1].astype(F32)
    s2k[...] = total.astype(BF16)
    for to in far:
        kz_copy(to).start()

    @pl.when(core == 0)
    def _():
        total = s1p[pl.ds(y * NZ, NZ)].astype(F32)
        for d in FAR_Y[::-1]:
            p1y_copy(d).wait_recv()
            total = total + r1a[d - 1].astype(F32)
        s2a[...] = total.astype(BF16)
        for to in far:
            p2z_copy(to).start()

    @pl.when(core == 1)
    def _():
        total = s1p[pl.ds(zlo * NY, NY)].astype(F32)
        for q in others:
            p1z_wait(q)
            total = total + r1b[q].astype(F32)
        s2b[...] = total.astype(BF16)
        for d in FAR_Y:
            p2y_copy(d).start()

    total = s2k[zlo].astype(F32)
    for q in others:
        kz_wait(q)
        total = total + r2k[q].astype(F32)
    keyv[...] = total[:OWN, :64]
    valv[...] = total[:OWN, 64:]

    a_swap.wait_send()
    for k in range(SPREAD):
        for d in range(1, NX):
            for e in range(NHALF):
                x_copy(e, d, k).wait_send()
        v_copy(k).wait_send()
        hp_copy(k).wait_send()
        for e in range(NHALF):
            h_copy(e, k).wait_send()
    for d in range(1, NY):
        ky_copy(d).wait_send()
    for q in others:
        kz_copy(q).wait_send()

    @pl.when(core == 0)
    def _():
        for d in range(1, NY):
            p1y_copy(d).wait_send()
        for q in others:
            p2z_copy(q).wait_send()

    @pl.when(core == 1)
    def _():
        for q in others:
            p1z_copy(q).wait_send()
        for d in range(1, NY):
            p2y_copy(d).wait_send()

    @pl.when(core == 0)
    def _():
        total = s2a[zlo].astype(F32)
        for q in others:
            p2z_wait(q)
            total = total + r2a[q].astype(F32)
        projv[...] = total[:OWN, :]

    @pl.when(core == 1)
    def _():
        total = s2b[y].astype(F32)
        for d in FAR_Y[::-1]:
            p2y_copy(d).wait_recv()
            total = total + r2b[d - 1].astype(F32)
        projv[...] = total[:OWN, :]


def writer(key_i, val_i, proj_i, hand_i, key_o, val_o, proj_o, hand_o, sem):
    pairs = ((key_i, key_o), (val_i, val_o), (proj_i, proj_o), (hand_i, hand_o))
    copies = [pltpu.make_async_copy(s, d, sem.at[i]) for i, (s, d) in enumerate(pairs)]
    for c in copies:
        c.start()
    for c in copies:
        c.wait()


def per_device(
    hidden_rows, key_grad, value_grad, visual_rows, visual_cotangent, norm_gain, norm_bias,
    fc1_weight, fc1_bias, fc2_weight, fc2_bias, layer_scale, token_counts, dest_offsets,
):
    anyspec = pl.BlockSpec(memory_space=pl.ANY)
    vmem = pl.BlockSpec(memory_space=pltpu.VMEM)
    dma = pltpu.SemaphoreType.DMA
    V = pltpu.VMEM
    S = pltpu.SMEM
    scratch = [
        V((512, WIDE), BF16), V((128, 512), BF16), V((256, 1024), BF16), V((4, 64, WIDE), BF16),
        V((1, 1024), F32), V((1, 1024), F32), V((1024, 512), BF16), V((1, 512), F32),
        V((512, 1024), BF16), V((1, 1024), F32), V((1, 1024), F32),
        S((1, IMAGES), jnp.int32), S((1, IMAGES), jnp.int32),
        V((256, 1024), BF16), V((NHALF, 256, 512), F32),
        V((NHALF, NX, SPREAD, CAP, 128), BF16), V((NHALF, NX - 1, SPREAD, CAP, 128), BF16),
        V((SPREAD, CAP, 128), BF16), V((SPREAD, CAP, 128), BF16),
        V((NHALF, SPREAD, CAP, 128), BF16), V((NHALF, SPREAD, CAP, 128), BF16),
        V((SPREAD, CAP, 128), BF16),
        V((WIDE + 80, 128), F32), V((NCORE, NY, NZ, BLK, 128), F32), V((NY, NZ, BLK, 128), F32),
        V((WIDE + 80, 256), F32), V((NCORE, N_CHIP * BLK, 256), BF16), V((N_CHIP * BLK, 256), BF16),
        V((N_CHIP * BLK, 128), F32),
        V((NY, NZ, BLK, 128), BF16), V((NY - 1, NZ, BLK, 128), BF16),
        V((NZ, BLK, 128), BF16), V((NZ, BLK, 128), BF16),
        V((N_CHIP, BLK, 128), BF16), V((NY - 1, NZ, BLK, 128), BF16), V((NZ, NY, BLK, 128), BF16),
        V((NZ, BLK, 128), BF16), V((NY, BLK, 128), BF16), V((NZ, BLK, 128), BF16), V((NY - 1, BLK, 128), BF16),
        dma((14,)), dma((2,)), dma((2,)), dma((SPREAD,)), dma((SPREAD,)),
        dma((NHALF, NX - 1, SPREAD)), dma((NHALF, NX - 1, SPREAD)), dma((SPREAD,)), dma((SPREAD,)),
        dma((NHALF, SPREAD)), dma((NHALF, SPREAD)),
        dma((NY - 1,)), dma((NY - 1,)), dma((NZ,)), dma((NZ,)),
        dma((NY - 1,)), dma((NY - 1,)), dma((NY - 1,)), dma((NY - 1,)), pltpu.SemaphoreType.REGULAR((2,)),
    ]
    shapes = (
        jax.ShapeDtypeStruct((OWN, 64), F32),
        jax.ShapeDtypeStruct((OWN, 64), F32),
        jax.ShapeDtypeStruct((OWN, 128), F32),
        jax.ShapeDtypeStruct((1, SPREAD, CAP, 128), BF16),
    )
    results = pl.pallas_call(
        kernel,
        out_shape=shapes,
        in_specs=[anyspec] * 14,
        out_specs=[vmem] * 4,
        scratch_shapes=scratch,
        compiler_params=pltpu.CompilerParams(
            collective_id=0, has_side_effects=True, vmem_limit_bytes=60 * 1024 * 1024
        ),
        name="bucket",
    )(
        hidden_rows, key_grad.T, value_grad.T, visual_rows, visual_cotangent,
        norm_gain.reshape(1, -1), norm_bias.reshape(1, -1), fc1_weight, fc1_bias.reshape(1, -1),
        fc2_weight, fc2_bias.reshape(1, -1), layer_scale.reshape(1, -1), token_counts, dest_offsets,
    )
    return pl.pallas_call(
        writer,
        out_shape=shapes,
        in_specs=[vmem] * 4,
        out_specs=[anyspec] * 4,
        scratch_shapes=[dma((4,))],
        name="writer",
    )(*results)


def solution(mesh):
    placed = (
        P("dp", None), P("dp", "mp"), P("dp", "mp"), P("dp", None), P("dp", None, None, None),
        P(), P(), P(None, "mp"), P("mp"), P("mp", None), P(), P(), P("dp", None), P("dp", None),
    )
    return jax.shard_map(
        per_device,
        mesh=mesh,
        in_specs=placed,
        out_specs=(P("dp", "mp"), P("dp", "mp"), P("dp", "mp"), P("dp", None, None, "mp")),
        check_vma=False,
    )
```

```python
import jax
import jax.numpy as jnp
from jax import lax
from jax.experimental import pallas as pl
from jax.experimental.pallas import tpu as pltpu
from jax.sharding import PartitionSpec as P

MESH = pl.DeviceIdType.MESH
F32 = jnp.float32
BF16 = jnp.bfloat16

NX, NY, NZ, NCORE, NHALF = 4, 8, 6, 2, 2
N_DP = NY * NZ * NCORE
N_CHIP = NY * NZ
SPREAD, CAP = 4, 64
SLOTS = SPREAD * CAP
IMAGES = 8
OWN = 38
BLK = 40
YROWS = NZ * NCORE * OWN
WIDE = 3584
FAR_Y = (4, 3, 5, 2, 6, 1, 7)
CHUNK = 4
GROUPS = ((0, 1), (1, 2), (3, 3))
EDGES = (0, NZ - 1)
FAR_Z = ((5, 4, 3, 2, 1), (5, 4, 3, 0, 2), (5, 4, 0, 3, 1), (0, 1, 5, 2, 4), (0, 1, 2, 5, 3), (0, 1, 2, 3, 4))


def kernel(
    hid_hbm, kgt_hbm, vgt_hbm, vis_hbm, cot_hbm, gain_hbm, nb_hbm, w1_hbm, b1_hbm, w2_hbm, b2_hbm, ls_hbm,
    cnt_hbm, off_hbm,
    keyv, valv, projv, hand,
    hid, kvt, vis, cot, vecs, w1, b1, w2, table,
    packed, hidden, part, xs, xr, vs, hs, got, hpar,
    kvf, kvo, kvp, cotf, amat, apar, half,
    s1k, r1k, s2k, r2k, s1p, r1y, r1z, s2z, s2y, r2z, r2y,
    lsem, swap_s, swap_r, x_s, x_r, got_s, got_r, k_s, k_r, p1y_s, p1y_r, p_s, p_r, go,
):
    dp = lax.axis_index("dp")
    mp = lax.axis_index("mp")
    core = lax.rem(dp, NCORE)
    chip = lax.div(dp, NCORE)
    zlo = lax.rem(chip, NZ)
    y = lax.div(chip, NZ)
    zhi = lax.div(mp, NX)
    x = lax.rem(mp, NX)
    partner = (dp + 1 - 2 * core, mp)

    def rank_of(y_, z_):
        return (y_ * NZ + z_) * NCORE + core

    def far_z(i):
        to = jnp.int32(0)
        for q in range(NZ):
            to = jnp.where(zlo == q, FAR_Z[q][i], to)
        return to

    far = [far_z(i) for i in range(NZ - 1)]

    def remote(src, dst, send, recv, who):
        return pltpu.make_async_remote_copy(
            src_ref=src, dst_ref=dst, send_sem=send, recv_sem=recv, device_id=who, device_id_type=MESH
        )

    def arrived(ref, sem):
        pltpu.make_async_copy(ref, ref, sem).wait()

    def load(i, *pairs):
        for src, dst in pairs:
            pltpu.make_async_copy(src, dst, lsem.at[i]).start()

    load(0, (cnt_hbm, table.at[0:1]), (off_hbm, table.at[1:2]))
    load(1, (vis_hbm, vis))
    load(2, *[(v, vecs.at[i : i + 1]) for i, v in enumerate((gain_hbm, nb_hbm, b2_hbm, ls_hbm))])
    load(3, (w1_hbm, w1))
    load(4, (b1_hbm, b1))
    load(5, (w2_hbm, w2))
    load(6, (kgt_hbm, kvt.at[0:64]), (vgt_hbm, kvt.at[64:128]))

    barrier = pltpu.get_barrier_semaphore()

    def greet(dp_, mp_):
        pl.semaphore_signal(barrier, 1, device_id=(dp_, mp_), device_id_type=MESH)

    for d in range(1, NX):
        greet(chip * NCORE, zhi * NX + lax.rem(x + d, NX))

    @pl.when(core == 1)
    def _():
        greet(chip * NCORE, mp)

    for d in range(1, NY):
        greet((lax.rem(y + d, NY) * NZ + zlo) * NCORE + 1, mp)
    for d in range(1, NZ):
        greet((y * NZ + lax.rem(zlo + d, NZ)) * NCORE + 1, mp)
    other = (1 - zhi) * NX + x
    for d in (0, 1, 2, N_CHIP - 1, N_CHIP - 2):
        there = lax.rem(chip + d, N_CHIP) * NCORE + 1
        if d:
            greet(there, mp)
        greet(there, other)
    near_count = 2 * (NX - 1) + 1
    far_count = 2 * (NY - 1 + NZ - 1 + 9)

    arrived(table, lsem.at[0])
    place = lax.broadcasted_iota(jnp.int32, (1, SLOTS), 1)
    target = jnp.full((1, SLOTS), -1, jnp.int32)
    counts = [table[0, i] for i in range(IMAGES)]
    offs = [table[1, i] for i in range(IMAGES)]
    start = jnp.int32(0)
    for i in range(IMAGES):
        end = start + counts[i]
        before = jnp.int32(0)
        for j in range(i):
            before = before + jnp.where(offs[j] == offs[i], counts[j], 0)
        base = (offs[i] - 1) * CAP + before - start
        inside = (place >= start) & (place < end)
        target = jnp.where(inside, place + base, target)
        start = end
    filled = []
    for k in range(1, SPREAD + 1):
        total = jnp.int32(0)
        for i in range(IMAGES):
            total = total + jnp.where(offs[i] == k, counts[i], 0)
        filled.append(total)
    slot_ids = lax.broadcasted_iota(jnp.int32, (SLOTS, SLOTS), 0)
    select = jnp.where(slot_ids == target, 1.0, 0.0).astype(BF16)

    def x_copy(e, d, k):
        to = lax.rem(x + d, NX)
        return remote(
            xs.at[e, to, k], xr.at[e, k, d - 1], x_s.at[0], x_r.at[e, k], (dp, zhi * NX + to)
        )

    def second(e, first, count):
        rows = slice(first * CAP, (first + count) * CAP)
        cols = pl.ds(pl.multiple_of(e * NX * 128, 128), NX * 128)
        res = jnp.dot(hidden[rows], w2[:, cols], preferred_element_type=F32)
        part[e, rows] = res
        for xd in range(NX):
            xs[e, xd, first : first + count] = (
                res[:, xd * 128 : (xd + 1) * 128].astype(BF16).reshape(count, CAP, 128)
            )

    def send_x(e, first, count):
        for k in range(first, first + count):
            for d in (2, 1, 3):
                x_copy(e, d, k).start()

    arrived(vis, lsem.at[1])
    for first in range(0, SPREAD, CHUNK):
        rows = slice(first * CAP, (first + CHUNK) * CAP)
        placed = jnp.dot(select[rows], vis[...], preferred_element_type=F32)
        packed[rows] = placed.astype(BF16)
        center = jnp.mean(placed, axis=1, keepdims=True)
        delta = placed - center
        spread_sq = jnp.mean(delta * delta, axis=1, keepdims=True)
        if first == 0:
            arrived(vecs, lsem.at[2])
        normed = (delta * lax.rsqrt(spread_sq + 1e-06) * vecs[0:1, :] + vecs[1:2, :]).astype(BF16)
        if first == 0:
            arrived(w1, lsem.at[3])
            arrived(b1, lsem.at[4])
            load(7, (hid_hbm, hid))
        pre = jnp.dot(normed, w1[...], preferred_element_type=F32) + b1[...]
        hidden[rows] = (0.5 * pre * (1.0 + lax.erf(pre * (0.5**0.5)))).astype(BF16)
        if first == 0:
            arrived(w2, lsem.at[5])
            load(8, (cot_hbm.at[0], cot))
        second(0, first, CHUNK)
        if first == 0:
            @pl.when(core == 0)
            def _():
                pl.semaphore_wait(barrier, near_count)
                pl.semaphore_signal(go.at[0], 1, device_id=partner, device_id_type=MESH)

            @pl.when(core == 1)
            def _():
                pl.semaphore_wait(go.at[0], 1)
        send_x(0, first, CHUNK)
    second(1, 0, SPREAD)
    send_x(1, 0, SPREAD)

    own_cols = pl.ds(pl.multiple_of(mp * 128, 128), 128)
    for k in range(SPREAD):
        vs[k] = packed[k * CAP : (k + 1) * CAP, own_cols]

    arrived(kvt, lsem.at[6])
    arrived(hid, lsem.at[7])
    kv = kvt[...].astype(F32).T.astype(BF16)

    @pl.loop(0, 7)
    def _(i):
        cols = pl.ds(pl.multiple_of(i * 512, 512), 512)
        kvf[cols, :] = lax.dot_general(
            hid[:, cols], kv, (((0,), (0,)), ((), ())), preferred_element_type=F32
        )

    colsum = jnp.sum(kv.astype(F32), axis=0, keepdims=True)
    tail_row = lax.broadcasted_iota(jnp.int32, (80, 128), 0)
    kvf[WIDE : WIDE + 80, :] = jnp.where(tail_row == 0, colsum, 0.0)

    @pl.loop(0, NY)
    def _(yy):
        win = kvf[pl.ds(pl.multiple_of(yy * YROWS, 8), YROWS + 8), :]
        for z in range(NZ):
            for c in range(NCORE):
                at = (z * NCORE + c) * OWN
                kvo[c, yy, z] = win[at : at + BLK, :]

    kv_swap = remote(kvo.at[1 - core], kvp, swap_s.at[0], swap_r.at[0], partner)
    kv_swap.start()

    def v_copy(k):
        return remote(vs.at[k], got.at[k, 2], got_s.at[0], got_r.at[k], (lax.rem(dp + k + 1, N_DP), mp))

    def h_copy(e, k):
        to = (lax.rem(dp + k + 1, N_DP), e * NX + x)
        return remote(hs.at[e, k], got.at[k, zhi], got_s.at[0], got_r.at[k], to)

    with_bias = jnp.where(zhi == 0, 1.0, 0.0)
    slot_in = lax.broadcasted_iota(jnp.int32, (CAP, 128), 0)
    @pl.when(core == 1)
    def _():
        pl.semaphore_wait(barrier, far_count)
        pl.semaphore_signal(go.at[1], 1, device_id=partner, device_id_type=MESH)

    @pl.when(core == 0)
    def _():
        pl.semaphore_wait(go.at[1], 1)

    def sum_x(e):
        cols = pl.ds(pl.multiple_of((e * NX + x) * 128, 128), 128)
        own = pl.ds(pl.multiple_of(x * 128, 128), 128)
        for k in range(SPREAD):
            arrived(xr.at[e, k], x_r.at[e, k])
            total = part[e, k * CAP : (k + 1) * CAP, own]
            for d in range(1, NX):
                total = total + xr[e, k, d - 1].astype(F32)
            branch = vecs[3:4, cols] * (total + with_bias * vecs[2:3, cols])
            hs[e, k] = jnp.where(slot_in < filled[k], branch, 0.0).astype(BF16)
            h_copy(e, k).start()

    def send_v():
        for k in range(SPREAD):
            v_copy(k).start()

    sum_x(0)
    pl.when(zhi == 0)(send_v)
    def ky_copy(d):
        to = lax.rem(y + d, NY)
        return remote(s1k.at[to], r1k.at[d - 1], k_s.at[0], k_r.at[0], (rank_of(to, zlo), mp))

    def from_z(to):
        return lax.rem(zlo - to + NZ, NZ) - 1

    def kz_copy(to):
        return remote(s2k.at[to], r2k.at[from_z(to)], k_s.at[1], k_r.at[1], (rank_of(y, to), mp))

    kv_swap.wait()

    @pl.loop(0, NY)
    def _(yy):
        s1k[yy] = (kvo[core, yy] + kvp[yy]).astype(BF16)

    for d in FAR_Y:
        ky_copy(d).start()

    sum_x(1)
    pl.when(zhi == 1)(send_v)

    arrived(cot, lsem.at[8])

    @pl.loop(0, 28)
    def _(i):
        cols = pl.ds(pl.multiple_of(i * 128, 128), 128)
        block = cot[:, :, cols].reshape(SLOTS, 128).astype(F32)
        cotf[cols, :] = block.T

    cotf[WIDE : WIDE + 80, :] = jnp.zeros((80, SLOTS), F32)

    @pl.loop(0, NY // 2)
    def _(j):
        win = cotf[pl.ds(pl.multiple_of(j * 2 * YROWS, 8), 2 * YROWS + 8), :]

        def block(yy, z, c):
            at = yy * YROWS + (z * NCORE + c) * OWN
            return win[at : at + BLK, :]

        for c in range(NCORE):
            for z in range(NZ):
                rows = jnp.concatenate([block(0, z, c), block(1, z, c)], axis=0).astype(BF16)
                amat[c, pl.ds(pl.multiple_of((z * NY + 2 * j) * BLK, 16), 2 * BLK), :] = rows

    a_swap = remote(amat.at[1 - core], apar, swap_s.at[1], swap_r.at[1], partner)
    a_swap.start()

    def hp_copy(k):
        return remote(hand.at[0, k], hpar.at[k], swap_s.at[2], swap_r.at[2], partner)

    for k in range(SPREAD):
        arrived(got.at[k], got_r.at[k])
        branch = got[k, 0].astype(F32) + got[k, 1].astype(F32)
        hand[0, k] = (got[k, 2].astype(F32) + branch).astype(BF16)
        hp_copy(k).start()

    half[...] = jnp.dot(amat[core], hand[0].reshape(SLOTS, 128), preferred_element_type=F32)

    a_swap.wait_recv()
    arrived(hpar, swap_r.at[2])

    theirs = hpar[...].reshape(SLOTS, 128)

    def p1y_copy(d, i, first, count):
        to = lax.rem(y + d, NY)
        zs = pl.ds(first, count)
        return remote(
            s1p.at[zs, to], r1y.at[d - 1, zs], p1y_s.at[i], p1y_r.at[i], (rank_of(to, zlo), mp)
        )

    def p1z_copy(to):
        return remote(s1p.at[to], r1z.at[from_z(to)], p_s.at[0], p_r.at[0], (rank_of(y, to), mp))

    def p2z_copy(to):
        return remote(s2z.at[to], r2z.at[from_z(to)], p_s.at[1], p_r.at[1], (rank_of(y, to), mp))

    def p2y_copy(d):
        to = lax.rem(y + d, NY)
        return remote(s2y.at[to], r2y.at[d - 1], p_s.at[2], p_r.at[2], (rank_of(to, zlo), mp))

    def block_rows(z):
        rows = pl.ds(pl.multiple_of(z * NY * BLK, 16), NY * BLK)
        res = half[rows, :] + jnp.dot(apar[rows, :], theirs, preferred_element_type=F32)
        s1p[z] = res.astype(BF16).reshape(NY, BLK, 128)

    inner = (zlo > 0) & (zlo < NZ - 1)
    z_first = (core == 1) & inner

    @pl.when(core == 0)
    def _():
        for i, (first, count) in enumerate(GROUPS):
            for z in range(first, first + count):
                block_rows(z)
            for d in FAR_Y:
                p1y_copy(d, i, first, count).start()

    @pl.when(core == 1)
    def _():
        for i, z in enumerate(EDGES):
            block_rows(z)
            for d in FAR_Y:
                p1y_copy(d, i, z, 1).start()
            if i == 0:
                for to in far:
                    @pl.when((to > 0) & (to < NZ - 1))
                    def _():
                        block_rows(to)
                        p1z_copy(to).start()

                @pl.when(inner)
                def _():
                    block_rows(zlo)

    total = s1k[y].astype(F32)
    arrived(r1k, k_r.at[0])
    for d in range(1, NY):
        total = total + r1k[d - 1].astype(F32)
    s2k[...] = total.astype(BF16)
    for to in far:
        kz_copy(to).start()

    def sum_y(i, first, count):
        total = s1p[first : first + count, y].astype(F32)
        arrived(r1y.at[:, pl.ds(first, count)], p1y_r.at[i])
        for d in range(1, NY):
            total = total + r1y[d - 1, first : first + count].astype(F32)
        s2z[first : first + count] = total.astype(BF16)
        for z in range(first, first + count):
            @pl.when(zlo != z)
            def _():
                p2z_copy(z).start()

    @pl.when(core == 0)
    def _():
        for i, (first, count) in enumerate(GROUPS):
            sum_y(i, first, count)

    @pl.when(core == 1)
    def _():
        sum_y(0, EDGES[0], 1)

        @pl.when(inner)
        def _():
            total = s1p[zlo].astype(F32)
            arrived(r1z, p_r.at[0])
            for d in range(1, NZ):
                total = total + r1z[d - 1].astype(F32)
            s2y[...] = total.astype(BF16)
            for d in FAR_Y:
                p2y_copy(d).start()

        sum_y(1, EDGES[1], 1)

    total = s2k[zlo].astype(F32)
    arrived(r2k, k_r.at[1])
    for d in range(1, NZ):
        total = total + r2k[d - 1].astype(F32)
    keyv[...] = total[:OWN, :64]
    valv[...] = total[:OWN, 64:]

    a_swap.wait_send()
    arrived(hpar, swap_s.at[2])
    arrived(xr, x_s.at[0])
    arrived(got, got_s.at[0])
    arrived(r1k, k_s.at[0])
    arrived(r2k, k_s.at[1])

    @pl.when(core == 0)
    def _():
        for i, (first, count) in enumerate(GROUPS):
            arrived(r1y.at[:, pl.ds(first, count)], p1y_s.at[i])
        arrived(r2z, p_s.at[1])

    @pl.when(core == 1)
    def _():
        for i, z in enumerate(EDGES):
            arrived(r1y.at[:, pl.ds(z, 1)], p1y_s.at[i])

        @pl.when(inner)
        def _():
            arrived(r1z.at[0 : NZ - 3], p_s.at[0])
            arrived(s2z.at[0:2], p_s.at[1])

        @pl.when(jnp.logical_not(inner))
        def _():
            arrived(r1z.at[0 : NZ - 2], p_s.at[0])
            arrived(s2z.at[0:1], p_s.at[1])

    @pl.when(z_first)
    def _():
        total = s2y[y].astype(F32)
        arrived(r2y, p_r.at[2])
        for d in range(1, NY):
            total = total + r2y[d - 1].astype(F32)
        projv[...] = total[:OWN, :]
        arrived(r2y, p_s.at[2])

    @pl.when(jnp.logical_not(z_first))
    def _():
        total = s2z[zlo].astype(F32)
        arrived(r2z, p_r.at[1])
        for d in range(1, NZ):
            total = total + r2z[d - 1].astype(F32)
        projv[...] = total[:OWN, :]


def writer(key_i, val_i, proj_i, hand_i, key_o, val_o, proj_o, hand_o, sem):
    pairs = ((key_i, key_o), (val_i, val_o), (proj_i, proj_o), (hand_i, hand_o))
    copies = [pltpu.make_async_copy(s, d, sem.at[i]) for i, (s, d) in enumerate(pairs)]
    for c in copies:
        c.start()
    for c in copies:
        c.wait()


def per_device(
    hidden_rows, key_grad, value_grad, visual_rows, visual_cotangent, norm_gain, norm_bias,
    fc1_weight, fc1_bias, fc2_weight, fc2_bias, layer_scale, token_counts, dest_offsets,
):
    anyspec = pl.BlockSpec(memory_space=pl.ANY)
    vmem = pl.BlockSpec(memory_space=pltpu.VMEM)
    dma = pltpu.SemaphoreType.DMA
    V = pltpu.VMEM
    S = pltpu.SMEM
    scratch = [
        V((512, WIDE), BF16), V((128, 512), BF16), V((256, 1024), BF16), V((4, 64, WIDE), BF16), V((4, 1024), F32),
        V((1024, 512), BF16), V((1, 512), F32), V((512, 1024), BF16), S((2, IMAGES), jnp.int32),
        V((256, 1024), BF16), V((256, 512), BF16), V((NHALF, 256, 512), F32),
        V((NHALF, NX, SPREAD, CAP, 128), BF16), V((NHALF, SPREAD, NX - 1, CAP, 128), BF16),
        V((SPREAD, CAP, 128), BF16), V((NHALF, SPREAD, CAP, 128), BF16), V((SPREAD, 3, CAP, 128), BF16),
        V((SPREAD, CAP, 128), BF16),
        V((WIDE + 80, 128), F32), V((NCORE, NY, NZ, BLK, 128), F32), V((NY, NZ, BLK, 128), F32),
        V((WIDE + 80, 256), F32), V((NCORE, N_CHIP * BLK, 256), BF16), V((N_CHIP * BLK, 256), BF16),
        V((N_CHIP * BLK, 128), F32),
        V((NY, NZ, BLK, 128), BF16), V((NY - 1, NZ, BLK, 128), BF16),
        V((NZ, BLK, 128), BF16), V((NZ - 1, BLK, 128), BF16),
        V((NZ, NY, BLK, 128), BF16), V((NY - 1, NZ, BLK, 128), BF16), V((NZ - 1, NY, BLK, 128), BF16),
        V((NZ, BLK, 128), BF16), V((NY, BLK, 128), BF16), V((NZ - 1, BLK, 128), BF16), V((NY - 1, BLK, 128), BF16),
        dma((9,)), dma((3,)), dma((3,)), dma((1,)), dma((NHALF, SPREAD)), dma((1,)), dma((SPREAD,)),
        dma((2,)), dma((2,)), dma((len(GROUPS),)), dma((len(GROUPS),)), dma((3,)), dma((3,)),
        pltpu.SemaphoreType.REGULAR((2,)),
    ]
    shapes = (
        jax.ShapeDtypeStruct((OWN, 64), F32),
        jax.ShapeDtypeStruct((OWN, 64), F32),
        jax.ShapeDtypeStruct((OWN, 128), F32),
        jax.ShapeDtypeStruct((1, SPREAD, CAP, 128), BF16),
    )
    held = (V((OWN, 64), F32), V((OWN, 64), F32), V((OWN, 128), F32), V((1, SPREAD, CAP, 128), BF16))
    results = pl.pallas_call(
        kernel,
        out_shape=held,
        in_specs=[anyspec] * 14,
        out_specs=[vmem] * 4,
        scratch_shapes=scratch,
        compiler_params=pltpu.CompilerParams(
            collective_id=0, has_side_effects=True, vmem_limit_bytes=60 * 1024 * 1024
        ),
        name="bucket",
    )(
        hidden_rows, key_grad.T, value_grad.T, visual_rows, visual_cotangent,
        norm_gain.reshape(1, -1), norm_bias.reshape(1, -1), fc1_weight, fc1_bias.reshape(1, -1),
        fc2_weight, fc2_bias.reshape(1, -1), layer_scale.reshape(1, -1), token_counts, dest_offsets,
    )
    return pl.pallas_call(
        writer,
        out_shape=shapes,
        in_specs=[vmem] * 4,
        out_specs=[anyspec] * 4,
        scratch_shapes=[dma((4,))],
        name="writer",
    )(*[pltpu.with_memory_space_constraint(r, pltpu.VMEM) for r in results])


def solution(mesh):
    placed = (
        P("dp", None), P("dp", "mp"), P("dp", "mp"), P("dp", None), P("dp", None, None, None),
        P(), P(), P(None, "mp"), P("mp"), P("mp", None), P(), P(), P("dp", None), P("dp", None),
    )
    return jax.shard_map(
        per_device,
        mesh=mesh,
        in_specs=placed,
        out_specs=(P("dp", "mp"), P("dp", "mp"), P("dp", "mp"), P("dp", None, None, "mp")),
        check_vma=False,
    )
```

```python
import jax
import jax.numpy as jnp
from jax import lax
from jax.experimental import pallas as pl
from jax.experimental.pallas import tpu as pltpu
from jax.sharding import PartitionSpec as P

MESH = pl.DeviceIdType.MESH
F32 = jnp.float32
BF16 = jnp.bfloat16

NX, NY, NZ, NCORE, NHALF = 4, 8, 6, 2, 2
N_DP = NY * NZ * NCORE
N_CHIP = NY * NZ
SPREAD, CAP = 4, 64
SLOTS = SPREAD * CAP
IMAGES = 8
OWN = 38
BLK = 40
YROWS = NZ * NCORE * OWN
WIDE = 3584
FAR_Y = (4, 3, 5, 2, 6, 1, 7)
LATE_Z = 4
CHUNK = 2
GROUPS = ((0, 1), (1, 2), (3, 3))
EDGES = (0, NZ - 1)
FAR_Z = ((5, 4, 3, 2, 1), (5, 4, 3, 0, 2), (5, 4, 0, 3, 1), (0, 1, 5, 2, 4), (0, 1, 2, 5, 3), (0, 1, 2, 3, 4))


def kernel(
    hid_hbm, kgt_hbm, vgt_hbm, vis_hbm, cot_hbm, gain_hbm, nb_hbm, w1_hbm, b1_hbm, w2_hbm, b2_hbm, ls_hbm,
    cnt_hbm, off_hbm,
    keyv, valv, projv, hand,
    hid, kvt, vis, cot, vecs, w1, b1, w2, table,
    packed, hidden, part, xs, xr, vs, hs, got, hpar,
    kvf, kvo, kvp, cotf, amat, apar, half,
    s1k, r1k, s2k, r2k, s1p, r1y, r1z, s2z, s2y, r2z, r2y,
    lsem, swap_s, swap_r, x_s, x_r, got_s, got_r, k_s, k_r, p1y_s, p1y_r, p_s, p_r, go,
):
    dp = lax.axis_index("dp")
    mp = lax.axis_index("mp")
    core = lax.rem(dp, NCORE)
    chip = lax.div(dp, NCORE)
    zlo = lax.rem(chip, NZ)
    y = lax.div(chip, NZ)
    zhi = lax.div(mp, NX)
    x = lax.rem(mp, NX)
    partner = (dp + 1 - 2 * core, mp)

    def rank_of(y_, z_):
        return (y_ * NZ + z_) * NCORE + core

    def far_z(i):
        to = jnp.int32(0)
        for q in range(NZ):
            to = jnp.where(zlo == q, FAR_Z[q][i], to)
        return to

    far = [far_z(i) for i in range(NZ - 1)]

    def remote(src, dst, send, recv, who):
        return pltpu.make_async_remote_copy(
            src_ref=src, dst_ref=dst, send_sem=send, recv_sem=recv, device_id=who, device_id_type=MESH
        )

    def arrived(ref, sem):
        pltpu.make_async_copy(ref, ref, sem).wait()

    def load(i, *pairs):
        for src, dst in pairs:
            pltpu.make_async_copy(src, dst, lsem.at[i]).start()

    load(0, (cnt_hbm, table.at[0:1]), (off_hbm, table.at[1:2]))
    load(1, (vis_hbm, vis))
    load(2, *[(v, vecs.at[i : i + 1]) for i, v in enumerate((gain_hbm, nb_hbm, b2_hbm, ls_hbm))])
    load(3, (w1_hbm, w1))
    load(4, (b1_hbm, b1))
    load(5, (w2_hbm, w2))
    load(6, (kgt_hbm, kvt.at[0:64]), (vgt_hbm, kvt.at[64:128]))

    barrier = pltpu.get_barrier_semaphore()
    even = x - lax.rem(x, 2)
    odd = even + 1
    ring = zhi * NX

    def signal(sem, dp_, mp_):
        pl.semaphore_signal(sem, 1, device_id=(dp_, mp_), device_id_type=MESH)

    for d in range(1, NX):
        signal(barrier, chip * NCORE, ring + lax.rem(x + d, NX))

    @pl.when(core == 1)
    def _():
        signal(barrier, chip * NCORE, mp)

    for d in range(1, NY):
        signal(barrier, (lax.rem(y + d, NY) * NZ + zlo) * NCORE + 1, ring + even)
    for d in range(1, NZ):
        signal(barrier, (y * NZ + lax.rem(zlo + d, NZ)) * NCORE + 1, ring + even)
    for d in (0, 1, 2, N_CHIP - 1, N_CHIP - 2):
        there = lax.rem(chip + d, N_CHIP) * NCORE + 1
        if d:
            signal(barrier, there, ring + even)
        signal(barrier, there, NX - ring + odd)

    def met(level, collects, count):
        hears = (core == 1) & (x == collects)

        @pl.when(hears)
        def _():
            pl.semaphore_wait(barrier, count)
            signal(go.at[level], chip * NCORE, mp)
            signal(go.at[level], chip * NCORE, ring + even + odd - x)
            signal(go.at[level], chip * NCORE + 1, ring + even + odd - x)

        @pl.when(jnp.logical_not(hears))
        def _():
            pl.semaphore_wait(go.at[level], 1)

    arrived(table, lsem.at[0])
    place = lax.broadcasted_iota(jnp.int32, (1, SLOTS), 1)
    target = jnp.full((1, SLOTS), -1, jnp.int32)
    counts = [table[0, i] for i in range(IMAGES)]
    offs = [table[1, i] for i in range(IMAGES)]
    start = jnp.int32(0)
    for i in range(IMAGES):
        end = start + counts[i]
        before = jnp.int32(0)
        for j in range(i):
            before = before + jnp.where(offs[j] == offs[i], counts[j], 0)
        base = (offs[i] - 1) * CAP + before - start
        inside = (place >= start) & (place < end)
        target = jnp.where(inside, place + base, target)
        start = end
    filled = []
    for k in range(1, SPREAD + 1):
        total = jnp.int32(0)
        for i in range(IMAGES):
            total = total + jnp.where(offs[i] == k, counts[i], 0)
        filled.append(total)
    slot_ids = lax.broadcasted_iota(jnp.int32, (SLOTS, SLOTS), 0)
    select = jnp.where(slot_ids == target, 1.0, 0.0).astype(BF16)

    def x_copy(e, d, k):
        to = lax.rem(x + d, NX)
        return remote(
            xs.at[e, to, k], xr.at[e, k, d - 1], x_s.at[0], x_r.at[e, k], (dp, zhi * NX + to)
        )

    def second(e, first, count):
        rows = slice(first * CAP, (first + count) * CAP)
        cols = pl.ds(pl.multiple_of(e * NX * 128, 128), NX * 128)
        res = jnp.dot(hidden[rows], w2[:, cols], preferred_element_type=F32)
        part[e, rows] = res
        for xd in range(NX):
            xs[e, xd, first : first + count] = (
                res[:, xd * 128 : (xd + 1) * 128].astype(BF16).reshape(count, CAP, 128)
            )

    def send_x(e, first, count):
        for k in range(first, first + count):
            for d in (2, 1, 3):
                x_copy(e, d, k).start()

    arrived(vis, lsem.at[1])
    for first in range(0, SPREAD, CHUNK):
        rows = slice(first * CAP, (first + CHUNK) * CAP)
        placed = jnp.dot(select[rows], vis[...], preferred_element_type=F32)
        packed[rows] = placed.astype(BF16)
        center = jnp.mean(placed, axis=1, keepdims=True)
        delta = placed - center
        spread_sq = jnp.mean(delta * delta, axis=1, keepdims=True)
        if first == 0:
            arrived(vecs, lsem.at[2])
        normed = (delta * lax.rsqrt(spread_sq + 1e-06) * vecs[0:1, :] + vecs[1:2, :]).astype(BF16)
        if first == 0:
            arrived(w1, lsem.at[3])
            arrived(b1, lsem.at[4])
            load(7, (hid_hbm, hid))
        pre = jnp.dot(normed, w1[...], preferred_element_type=F32) + b1[...]
        hidden[rows] = (0.5 * pre * (1.0 + lax.erf(pre * (0.5**0.5)))).astype(BF16)
        if first == 0:
            arrived(w2, lsem.at[5])
            load(8, (cot_hbm.at[0], cot))
        second(0, first, CHUNK)
        if first == 0:
            @pl.when(core == 0)
            def _():
                pl.semaphore_wait(barrier, 2 * (NX - 1) + 1)
                pl.semaphore_signal(go.at[0], 1, device_id=partner, device_id_type=MESH)

            @pl.when(core == 1)
            def _():
                pl.semaphore_wait(go.at[0], 1)
        send_x(0, first, CHUNK)
    second(1, 0, SPREAD)
    send_x(1, 0, SPREAD)

    own_cols = pl.ds(pl.multiple_of(mp * 128, 128), 128)
    for k in range(SPREAD):
        vs[k] = packed[k * CAP : (k + 1) * CAP, own_cols]

    def v_copy(k):
        return remote(vs.at[k], got.at[k, 2], got_s.at[0], got_r.at[k], (lax.rem(dp + k + 1, N_DP), mp))

    def h_copy(e, k):
        to = (lax.rem(dp + k + 1, N_DP), e * NX + x)
        return remote(hs.at[e, k], got.at[k, zhi], got_s.at[0], got_r.at[k], to)

    def send_v():
        for k in range(SPREAD):
            v_copy(k).start()

    def own_half_in():
        met(1, even, 4 * (NY - 1 + NZ - 1 + 4))

    def other_half_in():
        met(2, odd, 4 * 5)

    @pl.when((zhi == 0) & (zlo >= LATE_Z))
    def _():
        own_half_in()
        send_v()

    arrived(kvt, lsem.at[6])
    arrived(hid, lsem.at[7])
    kv = kvt[...].astype(F32).T.astype(BF16)

    @pl.loop(0, 7)
    def _(i):
        cols = pl.ds(pl.multiple_of(i * 512, 512), 512)
        kvf[cols, :] = lax.dot_general(
            hid[:, cols], kv, (((0,), (0,)), ((), ())), preferred_element_type=F32
        )

    colsum = jnp.sum(kv.astype(F32), axis=0, keepdims=True)
    tail_row = lax.broadcasted_iota(jnp.int32, (80, 128), 0)
    kvf[WIDE : WIDE + 80, :] = jnp.where(tail_row == 0, colsum, 0.0)

    @pl.loop(0, NY)
    def _(yy):
        win = kvf[pl.ds(pl.multiple_of(yy * YROWS, 8), YROWS + 8), :]
        for z in range(NZ):
            for c in range(NCORE):
                at = (z * NCORE + c) * OWN
                kvo[c, yy, z] = win[at : at + BLK, :]

    kv_swap = remote(kvo.at[1 - core], kvp, swap_s.at[0], swap_r.at[0], partner)
    kv_swap.start()

    with_bias = jnp.where(zhi == 0, 1.0, 0.0)
    slot_in = lax.broadcasted_iota(jnp.int32, (CAP, 128), 0)
    def ky_copy(d):
        to = lax.rem(y + d, NY)
        return remote(s1k.at[to], r1k.at[d - 1], k_s.at[0], k_r.at[0], (rank_of(to, zlo), mp))

    def from_z(to):
        return lax.rem(zlo - to + NZ, NZ) - 1

    def kz_copy(to):
        return remote(s2k.at[to], r2k.at[from_z(to)], k_s.at[1], k_r.at[1], (rank_of(y, to), mp))

    def send_kv():
        kv_swap.wait()

        @pl.loop(0, NY)
        def _(yy):
            s1k[yy] = (kvo[core, yy] + kvp[yy]).astype(BF16)

        for d in FAR_Y:
            ky_copy(d).start()

    @pl.when((zhi == 0) & (zlo < LATE_Z))
    def _():
        own_half_in()
        send_v()

    @pl.when(zhi == 1)
    def _():
        own_half_in()
        other_half_in()

    def sum_x(e):
        cols = pl.ds(pl.multiple_of((e * NX + x) * 128, 128), 128)
        own = pl.ds(pl.multiple_of(x * 128, 128), 128)
        for k in range(SPREAD):
            arrived(xr.at[e, k], x_r.at[e, k])
            total = part[e, k * CAP : (k + 1) * CAP, own]
            for d in range(1, NX):
                total = total + xr[e, k, d - 1].astype(F32)
            branch = vecs[3:4, cols] * (total + with_bias * vecs[2:3, cols])
            hs[e, k] = jnp.where(slot_in < filled[k], branch, 0.0).astype(BF16)
            h_copy(e, k).start()

    sum_x(0)
    send_kv()

    @pl.when(zhi == 1)
    def _():
        sum_x(1)
        send_v()

    arrived(cot, lsem.at[8])

    @pl.loop(0, 28)
    def _(i):
        cols = pl.ds(pl.multiple_of(i * 128, 128), 128)
        block = cot[:, :, cols].reshape(SLOTS, 128).astype(F32)
        cotf[cols, :] = block.T

    cotf[WIDE : WIDE + 80, :] = jnp.zeros((80, SLOTS), F32)

    @pl.loop(0, NY // 2)
    def _(j):
        win = cotf[pl.ds(pl.multiple_of(j * 2 * YROWS, 8), 2 * YROWS + 8), :]

        def block(yy, z, c):
            at = yy * YROWS + (z * NCORE + c) * OWN
            return win[at : at + BLK, :]

        for c in range(NCORE):
            for z in range(NZ):
                rows = jnp.concatenate([block(0, z, c), block(1, z, c)], axis=0).astype(BF16)
                amat[c, pl.ds(pl.multiple_of((z * NY + 2 * j) * BLK, 16), 2 * BLK), :] = rows

    a_swap = remote(amat.at[1 - core], apar, swap_s.at[1], swap_r.at[1], partner)
    a_swap.start()

    @pl.when(zhi == 0)
    def _():
        other_half_in()
        sum_x(1)

    def hp_copy(k):
        return remote(hand.at[0, k], hpar.at[k], swap_s.at[2], swap_r.at[2], partner)

    for k in range(SPREAD):
        arrived(got.at[k], got_r.at[k])
        branch = got[k, 0].astype(F32) + got[k, 1].astype(F32)
        hand[0, k] = (got[k, 2].astype(F32) + branch).astype(BF16)
        hp_copy(k).start()

    half[...] = jnp.dot(amat[core], hand[0].reshape(SLOTS, 128), preferred_element_type=F32)

    a_swap.wait_recv()
    arrived(hpar, swap_r.at[2])

    theirs = hpar[...].reshape(SLOTS, 128)

    def p1y_copy(d, i, first, count):
        to = lax.rem(y + d, NY)
        zs = pl.ds(first, count)
        return remote(
            s1p.at[zs, to], r1y.at[d - 1, zs], p1y_s.at[i], p1y_r.at[i], (rank_of(to, zlo), mp)
        )

    def p1z_copy(to):
        return remote(s1p.at[to], r1z.at[from_z(to)], p_s.at[0], p_r.at[0], (rank_of(y, to), mp))

    def p2z_copy(to):
        return remote(s2z.at[to], r2z.at[from_z(to)], p_s.at[1], p_r.at[1], (rank_of(y, to), mp))

    def p2y_copy(d):
        to = lax.rem(y + d, NY)
        return remote(s2y.at[to], r2y.at[d - 1], p_s.at[2], p_r.at[2], (rank_of(to, zlo), mp))

    def block_rows(z):
        rows = pl.ds(pl.multiple_of(z * NY * BLK, 16), NY * BLK)
        res = half[rows, :] + jnp.dot(apar[rows, :], theirs, preferred_element_type=F32)
        s1p[z] = res.astype(BF16).reshape(NY, BLK, 128)

    inner = (zlo > 0) & (zlo < NZ - 1)
    z_first = (core == 1) & inner

    @pl.when(core == 0)
    def _():
        for i, (first, count) in enumerate(GROUPS):
            for z in range(first, first + count):
                block_rows(z)
            for d in FAR_Y:
                p1y_copy(d, i, first, count).start()

    @pl.when(core == 1)
    def _():
        for i, z in enumerate(EDGES):
            block_rows(z)
            for d in FAR_Y:
                p1y_copy(d, i, z, 1).start()
            if i == 0:
                for to in far:
                    @pl.when((to > 0) & (to < NZ - 1))
                    def _():
                        block_rows(to)
                        p1z_copy(to).start()

                @pl.when(inner)
                def _():
                    block_rows(zlo)

    total = s1k[y].astype(F32)
    arrived(r1k, k_r.at[0])
    for d in range(1, NY):
        total = total + r1k[d - 1].astype(F32)
    s2k[...] = total.astype(BF16)
    for to in far:
        kz_copy(to).start()

    def sum_y(i, first, count):
        total = s1p[first : first + count, y].astype(F32)
        arrived(r1y.at[:, pl.ds(first, count)], p1y_r.at[i])
        for d in range(1, NY):
            total = total + r1y[d - 1, first : first + count].astype(F32)
        s2z[first : first + count] = total.astype(BF16)
        for z in range(first, first + count):
            @pl.when(zlo != z)
            def _():
                p2z_copy(z).start()

    @pl.when(core == 0)
    def _():
        for i, (first, count) in enumerate(GROUPS):
            sum_y(i, first, count)

    @pl.when(core == 1)
    def _():
        sum_y(0, EDGES[0], 1)

        @pl.when(inner)
        def _():
            total = s1p[zlo].astype(F32)
            arrived(r1z, p_r.at[0])
            for d in range(1, NZ):
                total = total + r1z[d - 1].astype(F32)
            s2y[...] = total.astype(BF16)
            for d in FAR_Y:
                p2y_copy(d).start()

        sum_y(1, EDGES[1], 1)

    total = s2k[zlo].astype(F32)
    arrived(r2k, k_r.at[1])
    for d in range(1, NZ):
        total = total + r2k[d - 1].astype(F32)
    keyv[...] = total[:OWN, :64]
    valv[...] = total[:OWN, 64:]

    a_swap.wait_send()
    arrived(hpar, swap_s.at[2])
    arrived(xr, x_s.at[0])
    arrived(got, got_s.at[0])
    arrived(r1k, k_s.at[0])
    arrived(r2k, k_s.at[1])

    @pl.when(core == 0)
    def _():
        for i, (first, count) in enumerate(GROUPS):
            arrived(r1y.at[:, pl.ds(first, count)], p1y_s.at[i])
        arrived(r2z, p_s.at[1])

    @pl.when(core == 1)
    def _():
        for i, z in enumerate(EDGES):
            arrived(r1y.at[:, pl.ds(z, 1)], p1y_s.at[i])

        @pl.when(inner)
        def _():
            arrived(r1z.at[0 : NZ - 3], p_s.at[0])
            arrived(s2z.at[0:2], p_s.at[1])

        @pl.when(jnp.logical_not(inner))
        def _():
            arrived(r1z.at[0 : NZ - 2], p_s.at[0])
            arrived(s2z.at[0:1], p_s.at[1])

    @pl.when(z_first)
    def _():
        total = s2y[y].astype(F32)
        arrived(r2y, p_r.at[2])
        for d in range(1, NY):
            total = total + r2y[d - 1].astype(F32)
        projv[...] = total[:OWN, :]
        arrived(r2y, p_s.at[2])

    @pl.when(jnp.logical_not(z_first))
    def _():
        total = s2z[zlo].astype(F32)
        arrived(r2z, p_r.at[1])
        for d in range(1, NZ):
            total = total + r2z[d - 1].astype(F32)
        projv[...] = total[:OWN, :]


def writer(key_i, val_i, proj_i, hand_i, key_o, val_o, proj_o, hand_o, sem):
    pairs = ((key_i, key_o), (val_i, val_o), (proj_i, proj_o), (hand_i, hand_o))
    copies = [pltpu.make_async_copy(s, d, sem.at[i]) for i, (s, d) in enumerate(pairs)]
    for c in copies:
        c.start()
    for c in copies:
        c.wait()


def per_device(
    hidden_rows, key_grad, value_grad, visual_rows, visual_cotangent, norm_gain, norm_bias,
    fc1_weight, fc1_bias, fc2_weight, fc2_bias, layer_scale, token_counts, dest_offsets,
):
    anyspec = pl.BlockSpec(memory_space=pl.ANY)
    vmem = pl.BlockSpec(memory_space=pltpu.VMEM)
    dma = pltpu.SemaphoreType.DMA
    V = pltpu.VMEM
    S = pltpu.SMEM
    scratch = [
        V((512, WIDE), BF16), V((128, 512), BF16), V((256, 1024), BF16), V((4, 64, WIDE), BF16), V((4, 1024), F32),
        V((1024, 512), BF16), V((1, 512), F32), V((512, 1024), BF16), S((2, IMAGES), jnp.int32),
        V((256, 1024), BF16), V((256, 512), BF16), V((NHALF, 256, 512), F32),
        V((NHALF, NX, SPREAD, CAP, 128), BF16), V((NHALF, SPREAD, NX - 1, CAP, 128), BF16),
        V((SPREAD, CAP, 128), BF16), V((NHALF, SPREAD, CAP, 128), BF16), V((SPREAD, 3, CAP, 128), BF16),
        V((SPREAD, CAP, 128), BF16),
        V((WIDE + 80, 128), F32), V((NCORE, NY, NZ, BLK, 128), F32), V((NY, NZ, BLK, 128), F32),
        V((WIDE + 80, 256), F32), V((NCORE, N_CHIP * BLK, 256), BF16), V((N_CHIP * BLK, 256), BF16),
        V((N_CHIP * BLK, 128), F32),
        V((NY, NZ, BLK, 128), BF16), V((NY - 1, NZ, BLK, 128), BF16),
        V((NZ, BLK, 128), BF16), V((NZ - 1, BLK, 128), BF16),
        V((NZ, NY, BLK, 128), BF16), V((NY - 1, NZ, BLK, 128), BF16), V((NZ - 1, NY, BLK, 128), BF16),
        V((NZ, BLK, 128), BF16), V((NY, BLK, 128), BF16), V((NZ - 1, BLK, 128), BF16), V((NY - 1, BLK, 128), BF16),
        dma((9,)), dma((3,)), dma((3,)), dma((1,)), dma((NHALF, SPREAD)), dma((1,)), dma((SPREAD,)),
        dma((2,)), dma((2,)), dma((len(GROUPS),)), dma((len(GROUPS),)), dma((3,)), dma((3,)),
        pltpu.SemaphoreType.REGULAR((3,)),
    ]
    shapes = (
        jax.ShapeDtypeStruct((OWN, 64), F32),
        jax.ShapeDtypeStruct((OWN, 64), F32),
        jax.ShapeDtypeStruct((OWN, 128), F32),
        jax.ShapeDtypeStruct((1, SPREAD, CAP, 128), BF16),
    )
    held = (V((OWN, 64), F32), V((OWN, 64), F32), V((OWN, 128), F32), V((1, SPREAD, CAP, 128), BF16))
    results = pl.pallas_call(
        kernel,
        out_shape=held,
        in_specs=[anyspec] * 14,
        out_specs=[vmem] * 4,
        scratch_shapes=scratch,
        compiler_params=pltpu.CompilerParams(
            collective_id=0, has_side_effects=True, vmem_limit_bytes=60 * 1024 * 1024
        ),
        name="bucket",
    )(
        hidden_rows, key_grad.T, value_grad.T, visual_rows, visual_cotangent,
        norm_gain.reshape(1, -1), norm_bias.reshape(1, -1), fc1_weight, fc1_bias.reshape(1, -1),
        fc2_weight, fc2_bias.reshape(1, -1), layer_scale.reshape(1, -1), token_counts, dest_offsets,
    )
    return pl.pallas_call(
        writer,
        out_shape=shapes,
        in_specs=[vmem] * 4,
        out_specs=[anyspec] * 4,
        scratch_shapes=[dma((4,))],
        name="writer",
    )(*[pltpu.with_memory_space_constraint(r, pltpu.VMEM) for r in results])


def solution(mesh):
    placed = (
        P("dp", None), P("dp", "mp"), P("dp", "mp"), P("dp", None), P("dp", None, None, None),
        P(), P(), P(None, "mp"), P("mp"), P("mp", None), P(), P(), P("dp", None), P("dp", None),
    )
    return jax.shard_map(
        per_device,
        mesh=mesh,
        in_specs=placed,
        out_specs=(P("dp", "mp"), P("dp", "mp"), P("dp", "mp"), P("dp", None, None, "mp")),
        check_vma=False,
    )
```

```python
import jax
import jax.numpy as jnp
from jax import lax
from jax.experimental import pallas as pl
from jax.experimental.pallas import tpu as pltpu
from jax.sharding import PartitionSpec as P

MESH = pl.DeviceIdType.MESH
F32 = jnp.float32
BF16 = jnp.bfloat16

NX, NY, NZ, NCORE, NHALF = 4, 8, 6, 2, 2
N_DP = NY * NZ * NCORE
N_CHIP = NY * NZ
SPREAD, CAP = 4, 64
SLOTS = SPREAD * CAP
IMAGES = 8
OWN = 38
BLK = 40
YROWS = NZ * NCORE * OWN
WIDE = 3584
FAR_Y = (4, 3, 5, 2, 6, 1, 7)
LATE_Z = 4
CHUNK = 2
Y_GROUPS = (((0, 1), (1, 1), (2, 2), (4, 2)), ((0, 1), (5, 1)))
Z_FIRST = ((), (1, 2, 3, 4))
SENDS = (
    (('y', 0), ('y', 1), ('y', 2), ('y', 3)),
    (('y', 0), ('z', 1), ('z', 2), ('z', 3), ('z', 4), ('y', 1)),
)
SUMS = (
    (('kv', 0), ('sum_y', 0), ('sum_y', 1), ('sum_y', 2), ('sum_y', 3)),
    (('sum_y', 0), ('kv', 0), ('sum_z', 0), ('sum_y', 1)),
)
N_GROUPS = max(len(groups) for groups in Y_GROUPS)
FAR_Z = ((5, 4, 3, 2, 1), (5, 4, 3, 0, 2), (5, 4, 0, 3, 1), (0, 1, 5, 2, 4), (0, 1, 2, 5, 3), (0, 1, 2, 3, 4))


def kernel(
    hid_hbm, kgt_hbm, vgt_hbm, vis_hbm, cot_hbm, gain_hbm, nb_hbm, w1_hbm, b1_hbm, w2_hbm, b2_hbm, ls_hbm,
    cnt_hbm, off_hbm,
    keyv, valv, projv, hand,
    hid, kvt, vis, cot, vecs, w1, b1, w2, table,
    packed, hidden, part, xs, xr, vs, hs, got, hpar,
    kvf, kvo, kvp, cotf, amat, apar, half,
    s1k, r1k, s2k, r2k, s1p, r1y, r1z, s2z, s2y, r2z, r2y,
    lsem, swap_s, swap_r, x_s, x_r, got_s, got_r, k_s, k_r, p1y_s, p1y_r, p_s, p_r, go,
):
    dp = lax.axis_index("dp")
    mp = lax.axis_index("mp")
    core = lax.rem(dp, NCORE)
    chip = lax.div(dp, NCORE)
    zlo = lax.rem(chip, NZ)
    y = lax.div(chip, NZ)
    zhi = lax.div(mp, NX)
    x = lax.rem(mp, NX)
    partner = (dp + 1 - 2 * core, mp)

    def rank_of(y_, z_):
        return (y_ * NZ + z_) * NCORE + core

    def far_z(i):
        to = jnp.int32(0)
        for q in range(NZ):
            to = jnp.where(zlo == q, FAR_Z[q][i], to)
        return to

    far = [far_z(i) for i in range(NZ - 1)]

    def remote(src, dst, send, recv, who):
        return pltpu.make_async_remote_copy(
            src_ref=src, dst_ref=dst, send_sem=send, recv_sem=recv, device_id=who, device_id_type=MESH
        )

    def arrived(ref, sem):
        pltpu.make_async_copy(ref, ref, sem).wait()

    def load(i, *pairs):
        for src, dst in pairs:
            pltpu.make_async_copy(src, dst, lsem.at[i]).start()

    load(0, (cnt_hbm, table.at[0:1]), (off_hbm, table.at[1:2]))
    load(1, (vis_hbm, vis))
    load(2, *[(v, vecs.at[i : i + 1]) for i, v in enumerate((gain_hbm, nb_hbm, b2_hbm, ls_hbm))])
    load(3, (w1_hbm, w1))
    load(4, (b1_hbm, b1))
    load(5, (w2_hbm, w2))
    load(6, (kgt_hbm, kvt.at[0:64]), (vgt_hbm, kvt.at[64:128]))

    barrier = pltpu.get_barrier_semaphore()
    even = x - lax.rem(x, 2)
    odd = even + 1
    ring = zhi * NX

    def signal(sem, dp_, mp_):
        pl.semaphore_signal(sem, 1, device_id=(dp_, mp_), device_id_type=MESH)

    for d in range(1, NX):
        signal(barrier, chip * NCORE, ring + lax.rem(x + d, NX))

    @pl.when(core == 1)
    def _():
        signal(barrier, chip * NCORE, mp)

    for d in range(1, NY):
        signal(barrier, (lax.rem(y + d, NY) * NZ + zlo) * NCORE + 1, ring + even)
    for d in range(1, NZ):
        signal(barrier, (y * NZ + lax.rem(zlo + d, NZ)) * NCORE + 1, ring + even)
    for d in (0, 1, 2, N_CHIP - 1, N_CHIP - 2):
        there = lax.rem(chip + d, N_CHIP) * NCORE + 1
        if d:
            signal(barrier, there, ring + even)
        signal(barrier, there, NX - ring + odd)

    def hears(collects):
        return (core == 1) & (x == collects)

    def hear(level, collects, count):
        @pl.when(hears(collects))
        def _():
            pl.semaphore_wait(barrier, count)
            signal(go.at[level], chip * NCORE, mp)
            signal(go.at[level], chip * NCORE, ring + even + odd - x)
            signal(go.at[level], chip * NCORE + 1, ring + even + odd - x)

    def heard(level, collects):
        @pl.when(jnp.logical_not(hears(collects)))
        def _():
            pl.semaphore_wait(go.at[level], 1)

    arrived(table, lsem.at[0])
    place = lax.broadcasted_iota(jnp.int32, (1, SLOTS), 1)
    target = jnp.full((1, SLOTS), -1, jnp.int32)
    counts = [table[0, i] for i in range(IMAGES)]
    offs = [table[1, i] for i in range(IMAGES)]
    start = jnp.int32(0)
    for i in range(IMAGES):
        end = start + counts[i]
        before = jnp.int32(0)
        for j in range(i):
            before = before + jnp.where(offs[j] == offs[i], counts[j], 0)
        base = (offs[i] - 1) * CAP + before - start
        inside = (place >= start) & (place < end)
        target = jnp.where(inside, place + base, target)
        start = end
    filled = []
    for k in range(1, SPREAD + 1):
        total = jnp.int32(0)
        for i in range(IMAGES):
            total = total + jnp.where(offs[i] == k, counts[i], 0)
        filled.append(total)
    slot_ids = lax.broadcasted_iota(jnp.int32, (SLOTS, SLOTS), 0)
    select = jnp.where(slot_ids == target, 1.0, 0.0).astype(BF16)

    def x_copy(e, d, k):
        to = lax.rem(x + d, NX)
        return remote(
            xs.at[e, to, k], xr.at[e, k, d - 1], x_s.at[0], x_r.at[e, k], (dp, zhi * NX + to)
        )

    def second(e, first, count):
        rows = slice(first * CAP, (first + count) * CAP)
        cols = pl.ds(pl.multiple_of(e * NX * 128, 128), NX * 128)
        res = jnp.dot(hidden[rows], w2[:, cols], preferred_element_type=F32)
        part[e, rows] = res
        for xd in range(NX):
            xs[e, xd, first : first + count] = (
                res[:, xd * 128 : (xd + 1) * 128].astype(BF16).reshape(count, CAP, 128)
            )

    def send_x(e, first, count):
        for k in range(first, first + count):
            for d in (2, 1, 3):
                x_copy(e, d, k).start()

    arrived(vis, lsem.at[1])
    for first in range(0, SPREAD, CHUNK):
        rows = slice(first * CAP, (first + CHUNK) * CAP)
        placed = jnp.dot(select[rows], vis[...], preferred_element_type=F32)
        packed[rows] = placed.astype(BF16)
        center = jnp.mean(placed, axis=1, keepdims=True)
        delta = placed - center
        spread_sq = jnp.mean(delta * delta, axis=1, keepdims=True)
        if first == 0:
            arrived(vecs, lsem.at[2])
        normed = (delta * lax.rsqrt(spread_sq + 1e-06) * vecs[0:1, :] + vecs[1:2, :]).astype(BF16)
        if first == 0:
            arrived(w1, lsem.at[3])
            arrived(b1, lsem.at[4])
            load(7, (hid_hbm, hid))
        pre = jnp.dot(normed, w1[...], preferred_element_type=F32) + b1[...]
        hidden[rows] = (0.5 * pre * (1.0 + lax.erf(pre * (0.5**0.5)))).astype(BF16)
        if first == 0:
            arrived(w2, lsem.at[5])
            load(8, (cot_hbm.at[0], cot))
        second(0, first, CHUNK)
        if first == 0:
            @pl.when(core == 0)
            def _():
                pl.semaphore_wait(barrier, 2 * (NX - 1) + 1)
                pl.semaphore_signal(go.at[0], 1, device_id=partner, device_id_type=MESH)

            @pl.when(core == 1)
            def _():
                pl.semaphore_wait(go.at[0], 1)
        send_x(0, first, CHUNK)
    second(1, 0, SPREAD)
    send_x(1, 0, SPREAD)

    own_cols = pl.ds(pl.multiple_of(mp * 128, 128), 128)
    for k in range(SPREAD):
        vs[k] = packed[k * CAP : (k + 1) * CAP, own_cols]

    def v_copy(k):
        return remote(vs.at[k], got.at[k, 2], got_s.at[0], got_r.at[k], (lax.rem(dp + k + 1, N_DP), mp))

    def h_copy(e, k):
        to = (lax.rem(dp + k + 1, N_DP), e * NX + x)
        return remote(hs.at[e, k], got.at[k, zhi], got_s.at[0], got_r.at[k], to)

    def send_v():
        for k in range(SPREAD):
            v_copy(k).start()

    own_half_in = (1, even, 4 * (NY - 1 + NZ - 1 + 4))
    other_half_in = (2, odd, 4 * 5)

    def met(level, collects, count):
        hear(level, collects, count)
        heard(level, collects)

    @pl.when((zhi == 0) & (zlo >= LATE_Z))
    def _():
        met(*own_half_in)
        send_v()

    arrived(kvt, lsem.at[6])
    arrived(hid, lsem.at[7])
    kv = kvt[...].astype(F32).T.astype(BF16)

    @pl.loop(0, 7)
    def _(i):
        cols = pl.ds(pl.multiple_of(i * 512, 512), 512)
        kvf[cols, :] = lax.dot_general(
            hid[:, cols], kv, (((0,), (0,)), ((), ())), preferred_element_type=F32
        )

    @pl.when(zhi == 1)
    def _():
        hear(*own_half_in)
        hear(*other_half_in)

    colsum = jnp.sum(kv.astype(F32), axis=0, keepdims=True)
    tail_row = lax.broadcasted_iota(jnp.int32, (80, 128), 0)
    kvf[WIDE : WIDE + 80, :] = jnp.where(tail_row == 0, colsum, 0.0)

    @pl.loop(0, NY)
    def _(yy):
        win = kvf[pl.ds(pl.multiple_of(yy * YROWS, 8), YROWS + 8), :]
        for z in range(NZ):
            for c in range(NCORE):
                at = (z * NCORE + c) * OWN
                kvo[c, yy, z] = win[at : at + BLK, :]

    kv_swap = remote(kvo.at[1 - core], kvp, swap_s.at[0], swap_r.at[0], partner)
    kv_swap.start()

    with_bias = jnp.where(zhi == 0, 1.0, 0.0)
    slot_in = lax.broadcasted_iota(jnp.int32, (CAP, 128), 0)
    def ky_copy(d):
        to = lax.rem(y + d, NY)
        return remote(s1k.at[to], r1k.at[d - 1], k_s.at[0], k_r.at[0], (rank_of(to, zlo), mp))

    def from_z(to):
        return lax.rem(zlo - to + NZ, NZ) - 1

    def kz_copy(to):
        return remote(s2k.at[to], r2k.at[from_z(to)], k_s.at[1], k_r.at[1], (rank_of(y, to), mp))

    def send_kv():
        kv_swap.wait()

        @pl.loop(0, NY)
        def _(yy):
            s1k[yy] = (kvo[core, yy] + kvp[yy]).astype(BF16)

        for d in FAR_Y:
            ky_copy(d).start()

    @pl.when((zhi == 0) & (zlo < LATE_Z))
    def _():
        met(*own_half_in)
        send_v()

    @pl.when(zhi == 1)
    def _():
        heard(1, even)
        heard(2, odd)

    def sum_x(e):
        cols = pl.ds(pl.multiple_of((e * NX + x) * 128, 128), 128)
        own = pl.ds(pl.multiple_of(x * 128, 128), 128)
        for k in range(SPREAD):
            arrived(xr.at[e, k], x_r.at[e, k])
            total = part[e, k * CAP : (k + 1) * CAP, own]
            for d in range(1, NX):
                total = total + xr[e, k, d - 1].astype(F32)
            branch = vecs[3:4, cols] * (total + with_bias * vecs[2:3, cols])
            hs[e, k] = jnp.where(slot_in < filled[k], branch, 0.0).astype(BF16)
            h_copy(e, k).start()

    sum_x(0)
    send_kv()

    @pl.when(zhi == 1)
    def _():
        sum_x(1)
        send_v()

    arrived(cot, lsem.at[8])

    @pl.loop(0, 28)
    def _(i):
        cols = pl.ds(pl.multiple_of(i * 128, 128), 128)
        block = cot[:, :, cols].reshape(SLOTS, 128).astype(F32)
        cotf[cols, :] = block.T

    cotf[WIDE : WIDE + 80, :] = jnp.zeros((80, SLOTS), F32)

    @pl.loop(0, NY // 2)
    def _(j):
        win = cotf[pl.ds(pl.multiple_of(j * 2 * YROWS, 8), 2 * YROWS + 8), :]

        def block(yy, z, c):
            at = yy * YROWS + (z * NCORE + c) * OWN
            return win[at : at + BLK, :]

        for c in range(NCORE):
            for z in range(NZ):
                rows = jnp.concatenate([block(0, z, c), block(1, z, c)], axis=0).astype(BF16)
                amat[c, pl.ds(pl.multiple_of((z * NY + 2 * j) * BLK, 16), 2 * BLK), :] = rows

    a_swap = remote(amat.at[1 - core], apar, swap_s.at[1], swap_r.at[1], partner)
    a_swap.start()

    @pl.when(zhi == 0)
    def _():
        met(*other_half_in)
        sum_x(1)

    def hp_copy(k):
        return remote(hand.at[0, k], hpar.at[k], swap_s.at[2], swap_r.at[2], partner)

    for k in range(SPREAD):
        arrived(got.at[k], got_r.at[k])
        branch = got[k, 0].astype(F32) + got[k, 1].astype(F32)
        hand[0, k] = (got[k, 2].astype(F32) + branch).astype(BF16)
        hp_copy(k).start()

    half[...] = jnp.dot(amat[core], hand[0].reshape(SLOTS, 128), preferred_element_type=F32)

    a_swap.wait_recv()
    arrived(hpar, swap_r.at[2])

    theirs = hpar[...].reshape(SLOTS, 128)

    def p1y_copy(d, i, first, count):
        to = lax.rem(y + d, NY)
        zs = pl.ds(first, count)
        return remote(
            s1p.at[zs, to], r1y.at[d - 1, zs], p1y_s.at[i], p1y_r.at[i], (rank_of(to, zlo), mp)
        )

    def p1z_copy(to):
        return remote(s1p.at[to], r1z.at[from_z(to)], p_s.at[0], p_r.at[0], (rank_of(y, to), mp))

    def p2z_copy(to):
        return remote(s2z.at[to], r2z.at[from_z(to)], p_s.at[1], p_r.at[1], (rank_of(y, to), mp))

    def p2y_copy(d):
        to = lax.rem(y + d, NY)
        return remote(s2y.at[to], r2y.at[d - 1], p_s.at[2], p_r.at[2], (rank_of(to, zlo), mp))

    def block_rows(z):
        rows = pl.ds(pl.multiple_of(z * NY * BLK, 16), NY * BLK)
        res = half[rows, :] + jnp.dot(apar[rows, :], theirs, preferred_element_type=F32)
        s1p[z] = res.astype(BF16).reshape(NY, BLK, 128)

    def kv_sum():
        total = s1k[y].astype(F32)
        arrived(r1k, k_r.at[0])
        for d in range(1, NY):
            total = total + r1k[d - 1].astype(F32)
        s2k[...] = total.astype(BF16)
        for to in far:
            kz_copy(to).start()

    def send_y(i, first, count):
        for z in range(first, first + count):
            block_rows(z)
        for d in FAR_Y:
            p1y_copy(d, i, first, count).start()

    def send_z(z):
        block_rows(z)

        @pl.when(zlo != z)
        def _():
            p1z_copy(z).start()

    def sum_y(i, first, count):
        total = s1p[first : first + count, y].astype(F32)
        arrived(r1y.at[:, pl.ds(first, count)], p1y_r.at[i])
        for d in range(1, NY):
            total = total + r1y[d - 1, first : first + count].astype(F32)
        s2z[first : first + count] = total.astype(BF16)
        for z in range(first, first + count):
            @pl.when(zlo != z)
            def _():
                p2z_copy(z).start()

    def one_of(zs):
        hit = zlo == zs[0]
        for z in zs[1:]:
            hit = hit | (zlo == z)
        return hit

    def sum_z(zs):
        @pl.when(one_of(zs))
        def _():
            total = s1p[zlo].astype(F32)
            arrived(r1z, p_r.at[0])
            for d in range(1, NZ):
                total = total + r1z[d - 1].astype(F32)
            s2y[...] = total.astype(BF16)
            for d in FAR_Y:
                p2y_copy(d).start()

    def follow(c, steps):
        groups, zs = Y_GROUPS[c], Z_FIRST[c]

        @pl.when(core == c)
        def _():
            for kind, i in steps:
                if kind == "kv":
                    kv_sum()
                elif kind == "sum_y":
                    sum_y(i, *groups[i])
                elif kind == "sum_z":
                    sum_z(zs)
                elif kind == "y":
                    send_y(i, *groups[i])
                else:
                    send_z(i)

    for c in range(NCORE):
        follow(c, SENDS[c])
    for c in range(NCORE):
        follow(c, SUMS[c])

    total = s2k[zlo].astype(F32)
    arrived(r2k, k_r.at[1])
    for d in range(1, NZ):
        total = total + r2k[d - 1].astype(F32)
    keyv[...] = total[:OWN, :64]
    valv[...] = total[:OWN, 64:]

    a_swap.wait_send()
    arrived(hpar, swap_s.at[2])
    arrived(xr, x_s.at[0])
    arrived(got, got_s.at[0])
    arrived(r1k, k_s.at[0])
    arrived(r2k, k_s.at[1])

    for c in range(NCORE):
        @pl.when(core == c)
        def _():
            zs = Z_FIRST[c]
            for i, (first, count) in enumerate(Y_GROUPS[c]):
                arrived(r1y.at[:, pl.ds(first, count)], p1y_s.at[i])
            if not zs:
                arrived(r2z, p_s.at[1])
                return
            mine = one_of(zs)

            @pl.when(mine)
            def _():
                if len(zs) > 1:
                    arrived(r1z.at[0 : len(zs) - 1], p_s.at[0])
                if len(zs) < NZ:
                    arrived(s2z.at[0 : NZ - len(zs)], p_s.at[1])

            @pl.when(jnp.logical_not(mine))
            def _():
                arrived(r1z.at[0 : len(zs)], p_s.at[0])
                if len(zs) < NZ - 1:
                    arrived(s2z.at[0 : NZ - len(zs) - 1], p_s.at[1])

    z_first = jnp.bool_(False)
    for c in range(NCORE):
        if Z_FIRST[c]:
            z_first = z_first | ((core == c) & one_of(Z_FIRST[c]))

    @pl.when(z_first)
    def _():
        total = s2y[y].astype(F32)
        arrived(r2y, p_r.at[2])
        for d in range(1, NY):
            total = total + r2y[d - 1].astype(F32)
        projv[...] = total[:OWN, :]
        arrived(r2y, p_s.at[2])

    @pl.when(jnp.logical_not(z_first))
    def _():
        total = s2z[zlo].astype(F32)
        arrived(r2z, p_r.at[1])
        for d in range(1, NZ):
            total = total + r2z[d - 1].astype(F32)
        projv[...] = total[:OWN, :]


def writer(key_i, val_i, proj_i, hand_i, key_o, val_o, proj_o, hand_o, sem):
    pairs = ((key_i, key_o), (val_i, val_o), (proj_i, proj_o), (hand_i, hand_o))
    copies = [pltpu.make_async_copy(s, d, sem.at[i]) for i, (s, d) in enumerate(pairs)]
    for c in copies:
        c.start()
    for c in copies:
        c.wait()


def per_device(
    hidden_rows, key_grad, value_grad, visual_rows, visual_cotangent, norm_gain, norm_bias,
    fc1_weight, fc1_bias, fc2_weight, fc2_bias, layer_scale, token_counts, dest_offsets,
):
    anyspec = pl.BlockSpec(memory_space=pl.ANY)
    vmem = pl.BlockSpec(memory_space=pltpu.VMEM)
    dma = pltpu.SemaphoreType.DMA
    V = pltpu.VMEM
    S = pltpu.SMEM
    scratch = [
        V((512, WIDE), BF16), V((128, 512), BF16), V((256, 1024), BF16), V((4, 64, WIDE), BF16), V((4, 1024), F32),
        V((1024, 512), BF16), V((1, 512), F32), V((512, 1024), BF16), S((2, IMAGES), jnp.int32),
        V((256, 1024), BF16), V((256, 512), BF16), V((NHALF, 256, 512), F32),
        V((NHALF, NX, SPREAD, CAP, 128), BF16), V((NHALF, SPREAD, NX - 1, CAP, 128), BF16),
        V((SPREAD, CAP, 128), BF16), V((NHALF, SPREAD, CAP, 128), BF16), V((SPREAD, 3, CAP, 128), BF16),
        V((SPREAD, CAP, 128), BF16),
        V((WIDE + 80, 128), F32), V((NCORE, NY, NZ, BLK, 128), F32), V((NY, NZ, BLK, 128), F32),
        V((WIDE + 80, 256), F32), V((NCORE, N_CHIP * BLK, 256), BF16), V((N_CHIP * BLK, 256), BF16),
        V((N_CHIP * BLK, 128), F32),
        V((NY, NZ, BLK, 128), BF16), V((NY - 1, NZ, BLK, 128), BF16),
        V((NZ, BLK, 128), BF16), V((NZ - 1, BLK, 128), BF16),
        V((NZ, NY, BLK, 128), BF16), V((NY - 1, NZ, BLK, 128), BF16), V((NZ - 1, NY, BLK, 128), BF16),
        V((NZ, BLK, 128), BF16), V((NY, BLK, 128), BF16), V((NZ - 1, BLK, 128), BF16), V((NY - 1, BLK, 128), BF16),
        dma((9,)), dma((3,)), dma((3,)), dma((1,)), dma((NHALF, SPREAD)), dma((1,)), dma((SPREAD,)),
        dma((2,)), dma((2,)), dma((N_GROUPS,)), dma((N_GROUPS,)), dma((3,)), dma((3,)),
        pltpu.SemaphoreType.REGULAR((3,)),
    ]
    shapes = (
        jax.ShapeDtypeStruct((OWN, 64), F32),
        jax.ShapeDtypeStruct((OWN, 64), F32),
        jax.ShapeDtypeStruct((OWN, 128), F32),
        jax.ShapeDtypeStruct((1, SPREAD, CAP, 128), BF16),
    )
    held = (V((OWN, 64), F32), V((OWN, 64), F32), V((OWN, 128), F32), V((1, SPREAD, CAP, 128), BF16))
    results = pl.pallas_call(
        kernel,
        out_shape=held,
        in_specs=[anyspec] * 14,
        out_specs=[vmem] * 4,
        scratch_shapes=scratch,
        compiler_params=pltpu.CompilerParams(
            collective_id=0, has_side_effects=True, vmem_limit_bytes=60 * 1024 * 1024
        ),
        name="bucket",
    )(
        hidden_rows, key_grad.T, value_grad.T, visual_rows, visual_cotangent,
        norm_gain.reshape(1, -1), norm_bias.reshape(1, -1), fc1_weight, fc1_bias.reshape(1, -1),
        fc2_weight, fc2_bias.reshape(1, -1), layer_scale.reshape(1, -1), token_counts, dest_offsets,
    )
    return pl.pallas_call(
        writer,
        out_shape=shapes,
        in_specs=[vmem] * 4,
        out_specs=[anyspec] * 4,
        scratch_shapes=[dma((4,))],
        name="writer",
    )(*[pltpu.with_memory_space_constraint(r, pltpu.VMEM) for r in results])


def solution(mesh):
    placed = (
        P("dp", None), P("dp", "mp"), P("dp", "mp"), P("dp", None), P("dp", None, None, None),
        P(), P(), P(None, "mp"), P("mp"), P("mp", None), P(), P(), P("dp", None), P("dp", None),
    )
    return jax.shard_map(
        per_device,
        mesh=mesh,
        in_specs=placed,
        out_specs=(P("dp", "mp"), P("dp", "mp"), P("dp", "mp"), P("dp", None, None, "mp")),
        check_vma=False,
    )
```

```python
import jax
import jax.numpy as jnp
from jax import lax
from jax.experimental import pallas as pl
from jax.experimental.pallas import tpu as pltpu
from jax.sharding import PartitionSpec as P

MESH = pl.DeviceIdType.MESH
F32 = jnp.float32
BF16 = jnp.bfloat16

NX, NY, NZ, NCORE, NHALF = 4, 8, 6, 2, 2
N_DP = NY * NZ * NCORE
N_CHIP = NY * NZ
SPREAD, CAP = 4, 64
SLOTS = SPREAD * CAP
IMAGES = 8
OWN = 38
BLK = 40
YROWS = NZ * NCORE * OWN
WIDE = 3584
FAR_Y = (4, 3, 5, 2, 6, 1, 7)
LATE_Z = 4
NORM_ROWS = 32
CHUNK = 2
Y_GROUPS = (((0, 1), (1, 1), (2, 2), (4, 2)), ((0, 1), (5, 1)))
Z_FIRST = ((), (1, 2, 3, 4))
SENDS = (
    (('y', 0), ('y', 1), ('y', 2), ('y', 3)),
    (('y', 0), ('z', 1), ('z', 2), ('z', 3), ('y', 1), ('z', 4)),
)
SUMS = (
    (('kv', 0), ('sum_y', 0), ('sum_y', 1), ('sum_y', 2), ('sum_y', 3)),
    (('sum_y', 0), ('kv', 0), ('sum_z', 0), ('sum_y', 1)),
)
N_GROUPS = max(len(groups) for groups in Y_GROUPS)
FAR_Z = ((5, 4, 3, 2, 1), (5, 4, 3, 0, 2), (5, 4, 0, 3, 1), (0, 1, 5, 2, 4), (0, 1, 2, 5, 3), (0, 1, 2, 3, 4))


def kernel(
    hid_hbm, kgt_hbm, vgt_hbm, vis_hbm, cot_hbm, gain_hbm, nb_hbm, w1_hbm, b1_hbm, w2_hbm, b2_hbm, ls_hbm,
    cnt_hbm, off_hbm,
    keyv, valv, projv, hand,
    hid, kvt, vis, cot, vecs, w1, b1, w2, table,
    packed, normed, hidden, part, xs, xr, vs, hs, got, hpar,
    kvf, kvo, kvp, cotf, amat, apar, half,
    s1k, r1k, s2k, r2k, s1p, r1y, r1z, s2z, s2y, r2z, r2y,
    lsem, swap_s, swap_r, x_s, x_r, got_s, got_r, k_s, k_r, p1y_s, p1y_r, p_s, p_r, go,
):
    dp = lax.axis_index("dp")
    mp = lax.axis_index("mp")
    core = lax.rem(dp, NCORE)
    chip = lax.div(dp, NCORE)
    zlo = lax.rem(chip, NZ)
    y = lax.div(chip, NZ)
    zhi = lax.div(mp, NX)
    x = lax.rem(mp, NX)
    partner = (dp + 1 - 2 * core, mp)

    def rank_of(y_, z_):
        return (y_ * NZ + z_) * NCORE + core

    def far_z(i):
        to = jnp.int32(0)
        for q in range(NZ):
            to = jnp.where(zlo == q, FAR_Z[q][i], to)
        return to

    far = [far_z(i) for i in range(NZ - 1)]

    def remote(src, dst, send, recv, who):
        return pltpu.make_async_remote_copy(
            src_ref=src, dst_ref=dst, send_sem=send, recv_sem=recv, device_id=who, device_id_type=MESH
        )

    def arrived(ref, sem):
        pltpu.make_async_copy(ref, ref, sem).wait()

    def load(i, *pairs):
        for src, dst in pairs:
            pltpu.make_async_copy(src, dst, lsem.at[i]).start()

    load(0, (cnt_hbm, table.at[0:1]), (off_hbm, table.at[1:2]))
    load(1, (vis_hbm, vis))
    load(2, *[(v, vecs.at[i : i + 1]) for i, v in enumerate((gain_hbm, nb_hbm, b2_hbm, ls_hbm))])
    load(3, (w1_hbm, w1))
    load(4, (b1_hbm, b1))
    load(5, (w2_hbm, w2))
    load(6, (kgt_hbm, kvt.at[0:64]), (vgt_hbm, kvt.at[64:128]))

    barrier = pltpu.get_barrier_semaphore()
    even = x - lax.rem(x, 2)
    odd = even + 1
    ring = zhi * NX

    def signal(sem, dp_, mp_):
        pl.semaphore_signal(sem, 1, device_id=(dp_, mp_), device_id_type=MESH)

    for d in range(1, NX):
        signal(barrier, chip * NCORE, ring + lax.rem(x + d, NX))

    @pl.when(core == 1)
    def _():
        signal(barrier, chip * NCORE, mp)

    for d in range(1, NY):
        signal(barrier, (lax.rem(y + d, NY) * NZ + zlo) * NCORE + 1, ring + even)
    for d in range(1, NZ):
        signal(barrier, (y * NZ + lax.rem(zlo + d, NZ)) * NCORE + 1, ring + even)
    for d in (0, 1, 2, N_CHIP - 1, N_CHIP - 2):
        there = lax.rem(chip + d, N_CHIP) * NCORE + 1
        if d:
            signal(barrier, there, ring + even)
        signal(barrier, there, NX - ring + odd)

    def hears(collects):
        return (core == 1) & (x == collects)

    def hear(level, collects, count):
        @pl.when(hears(collects))
        def _():
            pl.semaphore_wait(barrier, count)
            signal(go.at[level], chip * NCORE, mp)
            signal(go.at[level], chip * NCORE, ring + even + odd - x)
            signal(go.at[level], chip * NCORE + 1, ring + even + odd - x)

    def heard(level, collects):
        @pl.when(jnp.logical_not(hears(collects)))
        def _():
            pl.semaphore_wait(go.at[level], 1)

    arrived(table, lsem.at[0])
    place = lax.broadcasted_iota(jnp.int32, (1, SLOTS), 1)
    target = jnp.full((1, SLOTS), -1, jnp.int32)
    counts = [table[0, i] for i in range(IMAGES)]
    offs = [table[1, i] for i in range(IMAGES)]
    start = jnp.int32(0)
    for i in range(IMAGES):
        end = start + counts[i]
        before = jnp.int32(0)
        for j in range(i):
            before = before + jnp.where(offs[j] == offs[i], counts[j], 0)
        base = (offs[i] - 1) * CAP + before - start
        inside = (place >= start) & (place < end)
        target = jnp.where(inside, place + base, target)
        start = end
    filled = []
    for k in range(1, SPREAD + 1):
        total = jnp.int32(0)
        for i in range(IMAGES):
            total = total + jnp.where(offs[i] == k, counts[i], 0)
        filled.append(total)
    slot_ids = lax.broadcasted_iota(jnp.int32, (SLOTS, SLOTS), 0)
    select = jnp.where(slot_ids == target, 1.0, 0.0).astype(BF16)

    def x_copy(e, d, k):
        to = lax.rem(x + d, NX)
        return remote(
            xs.at[e, to, k], xr.at[e, k, d - 1], x_s.at[0], x_r.at[SPREAD if e else k], (dp, zhi * NX + to)
        )

    def second(e, first, count):
        rows = slice(first * CAP, (first + count) * CAP)
        cols = pl.ds(pl.multiple_of(e * NX * 128, 128), NX * 128)
        res = jnp.dot(hidden[rows], w2[:, cols], preferred_element_type=F32)
        part[e, rows] = res
        for xd in range(NX):
            xs[e, xd, first : first + count] = (
                res[:, xd * 128 : (xd + 1) * 128].astype(BF16).reshape(count, CAP, 128)
            )

    def send_x(e, first, count):
        for k in range(first, first + count):
            for d in (2, 1, 3):
                x_copy(e, d, k).start()

    arrived(vis, lsem.at[1])
    packed[...] = jnp.dot(select, vis[...], preferred_element_type=F32).astype(BF16)
    arrived(vecs, lsem.at[2])
    for at in range(0, SLOTS, NORM_ROWS):
        some = slice(at, at + NORM_ROWS)
        values = packed[some].astype(F32)
        center = jnp.mean(values, axis=1, keepdims=True)
        delta = values - center
        spread_sq = jnp.mean(delta * delta, axis=1, keepdims=True)
        normed[some] = (delta * lax.rsqrt(spread_sq + 1e-06) * vecs[0:1, :] + vecs[1:2, :]).astype(BF16)
    for first in range(0, SPREAD, CHUNK):
        rows = slice(first * CAP, (first + CHUNK) * CAP)
        if first == 0:
            arrived(w1, lsem.at[3])
            arrived(b1, lsem.at[4])
            load(7, (hid_hbm, hid))
        pre = jnp.dot(normed[rows], w1[...], preferred_element_type=F32) + b1[...]
        hidden[rows] = (0.5 * pre * (1.0 + lax.erf(pre * (0.5**0.5)))).astype(BF16)
        if first == 0:
            arrived(w2, lsem.at[5])
            load(8, (cot_hbm.at[0], cot))
        second(0, first, CHUNK)
        if first == 0:
            @pl.when(core == 0)
            def _():
                pl.semaphore_wait(barrier, 2 * (NX - 1) + 1)
                pl.semaphore_signal(go.at[0], 1, device_id=partner, device_id_type=MESH)

            @pl.when(core == 1)
            def _():
                pl.semaphore_wait(go.at[0], 1)
        send_x(0, first, CHUNK)
    second(1, 0, SPREAD)
    send_x(1, 0, SPREAD)

    own_cols = pl.ds(pl.multiple_of(mp * 128, 128), 128)
    for k in range(SPREAD):
        vs[k] = packed[k * CAP : (k + 1) * CAP, own_cols]

    def v_copy(k):
        return remote(vs.at[k], got.at[k, 2], got_s.at[0], got_r.at[k], (lax.rem(dp + k + 1, N_DP), mp))

    def h_copy(e, k):
        to = (lax.rem(dp + k + 1, N_DP), e * NX + x)
        return remote(hs.at[e, k], got.at[k, zhi], got_s.at[0], got_r.at[k], to)

    def send_v():
        for k in range(SPREAD):
            v_copy(k).start()

    own_half_in = (1, even, 4 * (NY - 1 + NZ - 1 + 4))
    other_half_in = (2, odd, 4 * 5)

    def met(level, collects, count):
        hear(level, collects, count)
        heard(level, collects)

    @pl.when((zhi == 0) & (zlo >= LATE_Z))
    def _():
        met(*own_half_in)
        send_v()

    arrived(kvt, lsem.at[6])
    arrived(hid, lsem.at[7])
    kv = kvt[...].astype(F32).T.astype(BF16)

    @pl.loop(0, 7)
    def _(i):
        cols = pl.ds(pl.multiple_of(i * 512, 512), 512)
        kvf[cols, :] = lax.dot_general(
            hid[:, cols], kv, (((0,), (0,)), ((), ())), preferred_element_type=F32
        )

    @pl.when(zhi == 1)
    def _():
        hear(*own_half_in)
        hear(*other_half_in)

    colsum = jnp.sum(kv.astype(F32), axis=0, keepdims=True)
    tail_row = lax.broadcasted_iota(jnp.int32, (80, 128), 0)
    kvf[WIDE : WIDE + 80, :] = jnp.where(tail_row == 0, colsum, 0.0)

    @pl.loop(0, NY)
    def _(yy):
        win = kvf[pl.ds(pl.multiple_of(yy * YROWS, 8), YROWS + 8), :]
        for z in range(NZ):
            for c in range(NCORE):
                at = (z * NCORE + c) * OWN
                kvo[c, yy, z] = win[at : at + BLK, :]

    kv_swap = remote(kvo.at[1 - core], kvp, swap_s.at[0], swap_r.at[0], partner)
    kv_swap.start()

    with_bias = jnp.where(zhi == 0, 1.0, 0.0)
    slot_in = lax.broadcasted_iota(jnp.int32, (CAP, 128), 0)
    def ky_copy(d):
        to = lax.rem(y + d, NY)
        return remote(s1k.at[to], r1k.at[d - 1], k_s.at[0], k_r.at[0], (rank_of(to, zlo), mp))

    def from_z(to):
        return lax.rem(zlo - to + NZ, NZ) - 1

    def kz_copy(to):
        return remote(s2k.at[to], r2k.at[from_z(to)], k_s.at[1], k_r.at[1], (rank_of(y, to), mp))

    def send_kv():
        kv_swap.wait()

        @pl.loop(0, NY)
        def _(yy):
            s1k[yy] = (kvo[core, yy] + kvp[yy]).astype(BF16)

        for d in FAR_Y:
            ky_copy(d).start()

    @pl.when((zhi == 0) & (zlo < LATE_Z))
    def _():
        met(*own_half_in)
        send_v()

    @pl.when(zhi == 1)
    def _():
        heard(1, even)
        heard(2, odd)

    def sum_x(e):
        cols = pl.ds(pl.multiple_of((e * NX + x) * 128, 128), 128)
        own = pl.ds(pl.multiple_of(x * 128, 128), 128)
        if e:
            arrived(xr.at[e], x_r.at[SPREAD])
        for k in range(SPREAD):
            if not e:
                arrived(xr.at[e, k], x_r.at[k])
            total = part[e, k * CAP : (k + 1) * CAP, own]
            for d in range(1, NX):
                total = total + xr[e, k, d - 1].astype(F32)
            branch = vecs[3:4, cols] * (total + with_bias * vecs[2:3, cols])
            hs[e, k] = jnp.where(slot_in < filled[k], branch, 0.0).astype(BF16)
            h_copy(e, k).start()

    sum_x(0)
    send_kv()

    @pl.when(zhi == 1)
    def _():
        sum_x(1)
        send_v()

    arrived(cot, lsem.at[8])

    @pl.loop(0, 28)
    def _(i):
        cols = pl.ds(pl.multiple_of(i * 128, 128), 128)
        block = cot[:, :, cols].reshape(SLOTS, 128).astype(F32)
        cotf[cols, :] = block.T

    cotf[WIDE : WIDE + 80, :] = jnp.zeros((80, SLOTS), F32)

    @pl.loop(0, NY // 2)
    def _(j):
        win = cotf[pl.ds(pl.multiple_of(j * 2 * YROWS, 8), 2 * YROWS + 8), :]

        def block(yy, z, c):
            at = yy * YROWS + (z * NCORE + c) * OWN
            return win[at : at + BLK, :]

        for c in range(NCORE):
            for z in range(NZ):
                rows = jnp.concatenate([block(0, z, c), block(1, z, c)], axis=0).astype(BF16)
                amat[c, pl.ds(pl.multiple_of((z * NY + 2 * j) * BLK, 16), 2 * BLK), :] = rows

    a_swap = remote(amat.at[1 - core], apar, swap_s.at[1], swap_r.at[1], partner)
    a_swap.start()

    @pl.when(zhi == 0)
    def _():
        met(*other_half_in)
        sum_x(1)

    def hp_copy(k):
        return remote(hand.at[0, k], hpar.at[k], swap_s.at[2], swap_r.at[2], partner)

    for k in range(SPREAD):
        arrived(got.at[k], got_r.at[k])
        branch = got[k, 0].astype(F32) + got[k, 1].astype(F32)
        hand[0, k] = (got[k, 2].astype(F32) + branch).astype(BF16)
        hp_copy(k).start()

    half[...] = jnp.dot(amat[core], hand[0].reshape(SLOTS, 128), preferred_element_type=F32)

    a_swap.wait_recv()
    arrived(hpar, swap_r.at[2])

    theirs = hpar[...].reshape(SLOTS, 128)

    def p1y_copy(d, i, first, count):
        to = lax.rem(y + d, NY)
        zs = pl.ds(first, count)
        return remote(
            s1p.at[zs, to], r1y.at[d - 1, zs], p1y_s.at[0], p1y_r.at[i], (rank_of(to, zlo), mp)
        )

    def p1z_copy(to):
        return remote(s1p.at[to], r1z.at[from_z(to)], p_s.at[0], p_r.at[0], (rank_of(y, to), mp))

    def p2z_copy(to):
        return remote(s2z.at[to], r2z.at[from_z(to)], p_s.at[1], p_r.at[1], (rank_of(y, to), mp))

    def p2y_copy(d):
        to = lax.rem(y + d, NY)
        return remote(s2y.at[to], r2y.at[d - 1], p_s.at[2], p_r.at[2], (rank_of(to, zlo), mp))

    def block_rows(z):
        rows = pl.ds(pl.multiple_of(z * NY * BLK, 16), NY * BLK)
        res = half[rows, :] + jnp.dot(apar[rows, :], theirs, preferred_element_type=F32)
        s1p[z] = res.astype(BF16).reshape(NY, BLK, 128)

    def kv_sum():
        total = s1k[y].astype(F32)
        arrived(r1k, k_r.at[0])
        for d in range(1, NY):
            total = total + r1k[d - 1].astype(F32)
        s2k[...] = total.astype(BF16)
        for to in far:
            kz_copy(to).start()

    def send_y(i, first, count):
        for z in range(first, first + count):
            block_rows(z)
        for d in FAR_Y:
            p1y_copy(d, i, first, count).start()

    def send_z(z):
        block_rows(z)

        @pl.when(zlo != z)
        def _():
            p1z_copy(z).start()

    def sum_y(i, first, count):
        total = s1p[first : first + count, y].astype(F32)
        arrived(r1y.at[:, pl.ds(first, count)], p1y_r.at[i])
        for d in range(1, NY):
            total = total + r1y[d - 1, first : first + count].astype(F32)
        s2z[first : first + count] = total.astype(BF16)
        for z in range(first, first + count):
            @pl.when(zlo != z)
            def _():
                p2z_copy(z).start()

    def one_of(zs):
        hit = zlo == zs[0]
        for z in zs[1:]:
            hit = hit | (zlo == z)
        return hit

    def sum_z(zs):
        @pl.when(one_of(zs))
        def _():
            total = s1p[zlo].astype(F32)
            arrived(r1z, p_r.at[0])
            for d in range(1, NZ):
                total = total + r1z[d - 1].astype(F32)
            s2y[...] = total.astype(BF16)
            for d in FAR_Y:
                p2y_copy(d).start()

    def follow(c, steps):
        groups, zs = Y_GROUPS[c], Z_FIRST[c]

        @pl.when(core == c)
        def _():
            for kind, i in steps:
                if kind == "kv":
                    kv_sum()
                elif kind == "sum_y":
                    sum_y(i, *groups[i])
                elif kind == "sum_z":
                    sum_z(zs)
                elif kind == "y":
                    send_y(i, *groups[i])
                else:
                    send_z(i)

    for c in range(NCORE):
        follow(c, SENDS[c])
    for c in range(NCORE):
        follow(c, SUMS[c])

    total = s2k[zlo].astype(F32)
    arrived(r2k, k_r.at[1])
    for d in range(1, NZ):
        total = total + r2k[d - 1].astype(F32)
    keyv[...] = total[:OWN, :64]
    valv[...] = total[:OWN, 64:]

    a_swap.wait_send()
    arrived(hpar, swap_s.at[2])
    arrived(xr, x_s.at[0])
    arrived(got, got_s.at[0])
    arrived(r1k, k_s.at[0])
    arrived(r2k, k_s.at[1])

    for c in range(NCORE):
        @pl.when(core == c)
        def _():
            zs = Z_FIRST[c]
            arrived(r1y.at[:, pl.ds(0, NZ - len(zs))], p1y_s.at[0])
            if not zs:
                arrived(r2z, p_s.at[1])
                return
            mine = one_of(zs)

            @pl.when(mine)
            def _():
                if len(zs) > 1:
                    arrived(r1z.at[0 : len(zs) - 1], p_s.at[0])
                if len(zs) < NZ:
                    arrived(s2z.at[0 : NZ - len(zs)], p_s.at[1])

            @pl.when(jnp.logical_not(mine))
            def _():
                arrived(r1z.at[0 : len(zs)], p_s.at[0])
                if len(zs) < NZ - 1:
                    arrived(s2z.at[0 : NZ - len(zs) - 1], p_s.at[1])

    z_first = jnp.bool_(False)
    for c in range(NCORE):
        if Z_FIRST[c]:
            z_first = z_first | ((core == c) & one_of(Z_FIRST[c]))

    @pl.when(z_first)
    def _():
        total = s2y[y].astype(F32)
        arrived(r2y, p_r.at[2])
        for d in range(1, NY):
            total = total + r2y[d - 1].astype(F32)
        projv[...] = total[:OWN, :]
        arrived(r2y, p_s.at[2])

    @pl.when(jnp.logical_not(z_first))
    def _():
        total = s2z[zlo].astype(F32)
        arrived(r2z, p_r.at[1])
        for d in range(1, NZ):
            total = total + r2z[d - 1].astype(F32)
        projv[...] = total[:OWN, :]


def writer(key_i, val_i, proj_i, hand_i, key_o, val_o, proj_o, hand_o, sem):
    pairs = ((key_i, key_o), (val_i, val_o), (proj_i, proj_o), (hand_i, hand_o))
    copies = [pltpu.make_async_copy(s, d, sem.at[i]) for i, (s, d) in enumerate(pairs)]
    for c in copies:
        c.start()
    for c in copies:
        c.wait()


def per_device(
    hidden_rows, key_grad, value_grad, visual_rows, visual_cotangent, norm_gain, norm_bias,
    fc1_weight, fc1_bias, fc2_weight, fc2_bias, layer_scale, token_counts, dest_offsets,
):
    anyspec = pl.BlockSpec(memory_space=pl.ANY)
    vmem = pl.BlockSpec(memory_space=pltpu.VMEM)
    dma = pltpu.SemaphoreType.DMA
    V = pltpu.VMEM
    S = pltpu.SMEM
    scratch = [
        V((512, WIDE), BF16), V((128, 512), BF16), V((256, 1024), BF16), V((4, 64, WIDE), BF16), V((4, 1024), F32),
        V((1024, 512), BF16), V((1, 512), F32), V((512, 1024), BF16), S((2, IMAGES), jnp.int32),
        V((256, 1024), BF16), V((256, 1024), BF16), V((256, 512), BF16), V((NHALF, 256, 512), F32),
        V((NHALF, NX, SPREAD, CAP, 128), BF16), V((NHALF, SPREAD, NX - 1, CAP, 128), BF16),
        V((SPREAD, CAP, 128), BF16), V((NHALF, SPREAD, CAP, 128), BF16), V((SPREAD, 3, CAP, 128), BF16),
        V((SPREAD, CAP, 128), BF16),
        V((WIDE + 80, 128), F32), V((NCORE, NY, NZ, BLK, 128), F32), V((NY, NZ, BLK, 128), F32),
        V((WIDE + 80, 256), F32), V((NCORE, N_CHIP * BLK, 256), BF16), V((N_CHIP * BLK, 256), BF16),
        V((N_CHIP * BLK, 128), F32),
        V((NY, NZ, BLK, 128), BF16), V((NY - 1, NZ, BLK, 128), BF16),
        V((NZ, BLK, 128), BF16), V((NZ - 1, BLK, 128), BF16),
        V((NZ, NY, BLK, 128), BF16), V((NY - 1, NZ, BLK, 128), BF16), V((NZ - 1, NY, BLK, 128), BF16),
        V((NZ, BLK, 128), BF16), V((NY, BLK, 128), BF16), V((NZ - 1, BLK, 128), BF16), V((NY - 1, BLK, 128), BF16),
        dma((9,)), dma((3,)), dma((3,)), dma((1,)), dma((SPREAD + 1,)), dma((1,)), dma((SPREAD,)),
        dma((2,)), dma((2,)), dma((1,)), dma((N_GROUPS,)), dma((3,)), dma((3,)),
        pltpu.SemaphoreType.REGULAR((3,)),
    ]
    shapes = (
        jax.ShapeDtypeStruct((OWN, 64), F32),
        jax.ShapeDtypeStruct((OWN, 64), F32),
        jax.ShapeDtypeStruct((OWN, 128), F32),
        jax.ShapeDtypeStruct((1, SPREAD, CAP, 128), BF16),
    )
    held = (V((OWN, 64), F32), V((OWN, 64), F32), V((OWN, 128), F32), V((1, SPREAD, CAP, 128), BF16))
    results = pl.pallas_call(
        kernel,
        out_shape=held,
        in_specs=[anyspec] * 14,
        out_specs=[vmem] * 4,
        scratch_shapes=scratch,
        compiler_params=pltpu.CompilerParams(
            collective_id=0, has_side_effects=True, vmem_limit_bytes=60 * 1024 * 1024
        ),
        name="bucket",
    )(
        hidden_rows, key_grad.T, value_grad.T, visual_rows, visual_cotangent,
        norm_gain.reshape(1, -1), norm_bias.reshape(1, -1), fc1_weight, fc1_bias.reshape(1, -1),
        fc2_weight, fc2_bias.reshape(1, -1), layer_scale.reshape(1, -1), token_counts, dest_offsets,
    )
    return pl.pallas_call(
        writer,
        out_shape=shapes,
        in_specs=[vmem] * 4,
        out_specs=[anyspec] * 4,
        scratch_shapes=[dma((4,))],
        name="writer",
    )(*[pltpu.with_memory_space_constraint(r, pltpu.VMEM) for r in results])


def solution(mesh):
    placed = (
        P("dp", None), P("dp", "mp"), P("dp", "mp"), P("dp", None), P("dp", None, None, None),
        P(), P(), P(None, "mp"), P("mp"), P("mp", None), P(), P(), P("dp", None), P("dp", None),
    )
    return jax.shard_map(
        per_device,
        mesh=mesh,
        in_specs=placed,
        out_specs=(P("dp", "mp"), P("dp", "mp"), P("dp", "mp"), P("dp", None, None, "mp")),
        check_vma=False,
    )
```

```python
import jax
import jax.numpy as jnp
from jax import lax
from jax.experimental import pallas as pl
from jax.experimental.pallas import tpu as pltpu
from jax.sharding import PartitionSpec as P

MESH = pl.DeviceIdType.MESH
F32 = jnp.float32
BF16 = jnp.bfloat16

NX, NY, NZ, NCORE, NHALF = 4, 8, 6, 2, 2
N_DP = NY * NZ * NCORE
N_CHIP = NY * NZ
SPREAD, CAP = 4, 64
SLOTS = SPREAD * CAP
IMAGES = 8
OWN = 38
BLK = 40
YROWS = NZ * NCORE * OWN
WIDE = 3584
FAR_Y = (4, 3, 5, 2, 6, 1, 7)
LATE_Z = 4
NORM_ROWS = 32
CHUNK = 2
Y_GROUPS = (((0, 1), (1, 1), (2, 2), (4, 2)), ((0, 1), (5, 1)))
Z_FIRST = ((), (1, 2, 3, 4))
SENDS = (
    (('y', 0), ('y', 1), ('y', 2), ('y', 3)),
    (('y', 0), ('z', 1), ('z', 2), ('z', 3), ('y', 1), ('z', 4)),
)
SUMS = (
    (('kv', 0), ('sum_y', 0), ('sum_y', 1), ('sum_y', 2), ('sum_y', 3)),
    (('sum_y', 0), ('kv', 0), ('sum_z', 0), ('sum_y', 1)),
)
N_GROUPS = max(len(groups) for groups in Y_GROUPS)
FAR_Z = ((5, 4, 3, 2, 1), (5, 4, 3, 0, 2), (5, 4, 0, 3, 1), (0, 1, 5, 2, 4), (0, 1, 2, 5, 3), (0, 1, 2, 3, 4))


def kernel(
    hid_hbm, kgt_hbm, vgt_hbm, vis_hbm, cot_hbm, gain_hbm, nb_hbm, w1_hbm, b1_hbm, w2_hbm, b2_hbm, ls_hbm,
    cnt_hbm, off_hbm,
    keyv, valv, projv, hand,
    hid, kvt, vis, cot, vecs, w1, b1, w2, table,
    packed, normed, hidden, part, xs, xr, vs, hs, got, hpar,
    kvf, kvo, kvp, cotf, amat, apar, half,
    s1k, r1k, s2k, r2k, s1p, r1y, r1z, s2z, s2y, r2z, r2y,
    lsem, swap_s, swap_r, x_s, x_r, got_s, got_r, k_s, k_r, p1y_s, p1y_r, p_s, p_r, go,
):
    dp = lax.axis_index("dp")
    mp = lax.axis_index("mp")
    core = lax.rem(dp, NCORE)
    chip = lax.div(dp, NCORE)
    zlo = lax.rem(chip, NZ)
    y = lax.div(chip, NZ)
    zhi = lax.div(mp, NX)
    x = lax.rem(mp, NX)
    partner = (dp + 1 - 2 * core, mp)

    def rank_of(y_, z_):
        return (y_ * NZ + z_) * NCORE + core

    def far_z(i):
        to = jnp.int32(0)
        for q in range(NZ):
            to = jnp.where(zlo == q, FAR_Z[q][i], to)
        return to

    far = [far_z(i) for i in range(NZ - 1)]

    def remote(src, dst, send, recv, who):
        return pltpu.make_async_remote_copy(
            src_ref=src, dst_ref=dst, send_sem=send, recv_sem=recv, device_id=who, device_id_type=MESH
        )

    def arrived(ref, sem):
        pltpu.make_async_copy(ref, ref, sem).wait()

    def load(i, *pairs):
        for src, dst in pairs:
            pltpu.make_async_copy(src, dst, lsem.at[i]).start()

    load(0, (cnt_hbm, table.at[0:1]), (off_hbm, table.at[1:2]))
    load(1, (vis_hbm, vis))
    load(2, *[(v, vecs.at[i : i + 1]) for i, v in enumerate((gain_hbm, nb_hbm, b2_hbm, ls_hbm))])
    load(3, (w1_hbm, w1))
    load(4, (b1_hbm, b1))
    load(5, (w2_hbm, w2))
    load(6, (kgt_hbm, kvt.at[0:64]), (vgt_hbm, kvt.at[64:128]))

    barrier = pltpu.get_barrier_semaphore()
    even = x - lax.rem(x, 2)
    odd = even + 1
    ring = zhi * NX

    def signal(sem, dp_, mp_):
        pl.semaphore_signal(sem, 1, device_id=(dp_, mp_), device_id_type=MESH)

    for d in range(1, NX):
        signal(barrier, chip * NCORE, ring + lax.rem(x + d, NX))

    @pl.when(core == 1)
    def _():
        signal(barrier, chip * NCORE, mp)

    for d in range(1, NY):
        signal(barrier, (lax.rem(y + d, NY) * NZ + zlo) * NCORE + 1, ring + even)
    for d in range(1, NZ):
        signal(barrier, (y * NZ + lax.rem(zlo + d, NZ)) * NCORE + 1, ring + even)
    for d in (0, 1, 2, N_CHIP - 1, N_CHIP - 2):
        there = lax.rem(chip + d, N_CHIP) * NCORE + 1
        if d:
            signal(barrier, there, ring + even)
        signal(barrier, there, NX - ring + odd)

    def hears(collects):
        return (core == 1) & (x == collects)

    def hear(level, collects, count):
        @pl.when(hears(collects))
        def _():
            pl.semaphore_wait(barrier, count)
            signal(go.at[level], chip * NCORE, mp)
            signal(go.at[level], chip * NCORE, ring + even + odd - x)
            signal(go.at[level], chip * NCORE + 1, ring + even + odd - x)

    def heard(level, collects):
        @pl.when(jnp.logical_not(hears(collects)))
        def _():
            pl.semaphore_wait(go.at[level], 1)

    arrived(table, lsem.at[0])
    place = lax.broadcasted_iota(jnp.int32, (1, SLOTS), 1)
    target = jnp.full((1, SLOTS), -1, jnp.int32)
    counts = [table[0, i] for i in range(IMAGES)]
    offs = [table[1, i] for i in range(IMAGES)]
    start = jnp.int32(0)
    for i in range(IMAGES):
        end = start + counts[i]
        before = jnp.int32(0)
        for j in range(i):
            before = before + jnp.where(offs[j] == offs[i], counts[j], 0)
        base = (offs[i] - 1) * CAP + before - start
        inside = (place >= start) & (place < end)
        target = jnp.where(inside, place + base, target)
        start = end
    filled = []
    for k in range(1, SPREAD + 1):
        total = jnp.int32(0)
        for i in range(IMAGES):
            total = total + jnp.where(offs[i] == k, counts[i], 0)
        filled.append(total)
    slot_ids = lax.broadcasted_iota(jnp.int32, (SLOTS, SLOTS), 0)
    select = jnp.where(slot_ids == target, 1.0, 0.0).astype(BF16)

    def x_copy(e, d, k):
        to = lax.rem(x + d, NX)
        return remote(
            xs.at[e, to, k], xr.at[e, k, d - 1], x_s.at[0], x_r.at[SPREAD if e else k], (dp, zhi * NX + to)
        )

    def second(e, first, count):
        rows = slice(first * CAP, (first + count) * CAP)
        cols = pl.ds(pl.multiple_of(e * NX * 128, 128), NX * 128)
        res = jnp.dot(hidden[rows], w2[:, cols], preferred_element_type=F32)
        part[e, rows] = res
        for xd in range(NX):
            xs[e, xd, first : first + count] = (
                res[:, xd * 128 : (xd + 1) * 128].astype(BF16).reshape(count, CAP, 128)
            )

    def send_x(e, first, count):
        for k in range(first, first + count):
            for d in (1, 3, 2):
                x_copy(e, d, k).start()

    arrived(vis, lsem.at[1])
    packed[...] = jnp.dot(select, vis[...], preferred_element_type=F32).astype(BF16)
    arrived(vecs, lsem.at[2])
    for at in range(0, SLOTS, NORM_ROWS):
        some = slice(at, at + NORM_ROWS)
        values = packed[some].astype(F32)
        center = jnp.mean(values, axis=1, keepdims=True)
        delta = values - center
        spread_sq = jnp.mean(delta * delta, axis=1, keepdims=True)
        normed[some] = (delta * lax.rsqrt(spread_sq + 1e-06) * vecs[0:1, :] + vecs[1:2, :]).astype(BF16)
    for first in range(0, SPREAD, CHUNK):
        rows = slice(first * CAP, (first + CHUNK) * CAP)
        if first == 0:
            arrived(w1, lsem.at[3])
            arrived(b1, lsem.at[4])
            load(7, (hid_hbm, hid))
        pre = jnp.dot(normed[rows], w1[...], preferred_element_type=F32) + b1[...]
        hidden[rows] = (0.5 * pre * (1.0 + lax.erf(pre * (0.5**0.5)))).astype(BF16)
        if first == 0:
            arrived(w2, lsem.at[5])
            load(8, (cot_hbm.at[0], cot))
        second(0, first, CHUNK)
        if first == 0:
            @pl.when(core == 0)
            def _():
                pl.semaphore_wait(barrier, 2 * (NX - 1) + 1)
                pl.semaphore_signal(go.at[0], 1, device_id=partner, device_id_type=MESH)

            @pl.when(core == 1)
            def _():
                pl.semaphore_wait(go.at[0], 1)
        send_x(0, first, CHUNK)
    second(1, 0, SPREAD)
    send_x(1, 0, SPREAD)

    own_cols = pl.ds(pl.multiple_of(mp * 128, 128), 128)
    for k in range(SPREAD):
        vs[k] = packed[k * CAP : (k + 1) * CAP, own_cols]

    def v_copy(k):
        return remote(vs.at[k], got.at[k, 2], got_s.at[0], got_r.at[k], (lax.rem(dp + k + 1, N_DP), mp))

    def h_copy(e, k):
        to = (lax.rem(dp + k + 1, N_DP), e * NX + x)
        return remote(hs.at[e, k], got.at[k, zhi], got_s.at[0], got_r.at[k], to)

    def send_v():
        for k in range(SPREAD):
            v_copy(k).start()

    own_half_in = (1, even, 4 * (NY - 1 + NZ - 1 + 4))
    other_half_in = (2, odd, 4 * 5)

    def met(level, collects, count):
        hear(level, collects, count)
        heard(level, collects)

    @pl.when((zhi == 0) & (zlo >= LATE_Z))
    def _():
        met(*own_half_in)
        send_v()

    arrived(kvt, lsem.at[6])
    arrived(hid, lsem.at[7])
    kv = kvt[...].astype(F32).T.astype(BF16)

    @pl.loop(0, 7)
    def _(i):
        cols = pl.ds(pl.multiple_of(i * 512, 512), 512)
        kvf[cols, :] = lax.dot_general(
            hid[:, cols], kv, (((0,), (0,)), ((), ())), preferred_element_type=F32
        )

    @pl.when(zhi == 1)
    def _():
        hear(*own_half_in)
        hear(*other_half_in)

    colsum = jnp.sum(kv.astype(F32), axis=0, keepdims=True)
    tail_row = lax.broadcasted_iota(jnp.int32, (80, 128), 0)
    kvf[WIDE : WIDE + 80, :] = jnp.where(tail_row == 0, colsum, 0.0)

    @pl.loop(0, NY)
    def _(yy):
        win = kvf[pl.ds(pl.multiple_of(yy * YROWS, 8), YROWS + 8), :]
        for z in range(NZ):
            for c in range(NCORE):
                at = (z * NCORE + c) * OWN
                kvo[c, yy, z] = win[at : at + BLK, :]

    kv_swap = remote(kvo.at[1 - core], kvp, swap_s.at[0], swap_r.at[0], partner)
    kv_swap.start()

    with_bias = jnp.where(zhi == 0, 1.0, 0.0)
    slot_in = lax.broadcasted_iota(jnp.int32, (CAP, 128), 0)
    def ky_copy(d):
        to = lax.rem(y + d, NY)
        return remote(s1k.at[to], r1k.at[d - 1], k_s.at[0], k_r.at[0], (rank_of(to, zlo), mp))

    def from_z(to):
        return lax.rem(zlo - to + NZ, NZ) - 1

    def kz_copy(to):
        return remote(s2k.at[to], r2k.at[from_z(to)], k_s.at[1], k_r.at[1], (rank_of(y, to), mp))

    def send_kv():
        kv_swap.wait()

        @pl.loop(0, NY)
        def _(yy):
            s1k[yy] = (kvo[core, yy] + kvp[yy]).astype(BF16)

        for d in FAR_Y:
            ky_copy(d).start()

    @pl.when((zhi == 0) & (zlo < LATE_Z))
    def _():
        met(*own_half_in)
        send_v()

    @pl.when(zhi == 1)
    def _():
        heard(1, even)
        heard(2, odd)

    def sum_x(e):
        cols = pl.ds(pl.multiple_of((e * NX + x) * 128, 128), 128)
        own = pl.ds(pl.multiple_of(x * 128, 128), 128)
        if e:
            arrived(xr.at[e], x_r.at[SPREAD])
        for k in range(SPREAD):
            if not e:
                arrived(xr.at[e, k], x_r.at[k])
            total = part[e, k * CAP : (k + 1) * CAP, own]
            for d in range(1, NX):
                total = total + xr[e, k, d - 1].astype(F32)
            branch = vecs[3:4, cols] * (total + with_bias * vecs[2:3, cols])
            hs[e, k] = jnp.where(slot_in < filled[k], branch, 0.0).astype(BF16)
            h_copy(e, k).start()

    sum_x(0)
    send_kv()

    @pl.when(zhi == 1)
    def _():
        sum_x(1)
        send_v()

    arrived(cot, lsem.at[8])

    @pl.loop(0, 28)
    def _(i):
        cols = pl.ds(pl.multiple_of(i * 128, 128), 128)
        block = cot[:, :, cols].reshape(SLOTS, 128).astype(F32)
        cotf[cols, :] = block.T

    cotf[WIDE : WIDE + 80, :] = jnp.zeros((80, SLOTS), F32)

    @pl.loop(0, NY // 2)
    def _(j):
        win = cotf[pl.ds(pl.multiple_of(j * 2 * YROWS, 8), 2 * YROWS + 8), :]

        def block(yy, z, c):
            at = yy * YROWS + (z * NCORE + c) * OWN
            return win[at : at + BLK, :]

        for c in range(NCORE):
            for z in range(NZ):
                rows = jnp.concatenate([block(0, z, c), block(1, z, c)], axis=0).astype(BF16)
                amat[c, pl.ds(pl.multiple_of((z * NY + 2 * j) * BLK, 16), 2 * BLK), :] = rows

    a_swap = remote(amat.at[1 - core], apar, swap_s.at[1], swap_r.at[1], partner)
    a_swap.start()

    @pl.when(zhi == 0)
    def _():
        met(*other_half_in)
        sum_x(1)

    def hp_copy(k):
        return remote(hand.at[0, k], hpar.at[k], swap_s.at[2], swap_r.at[2], partner)

    for k in range(SPREAD):
        arrived(got.at[k], got_r.at[k])
        branch = got[k, 0].astype(F32) + got[k, 1].astype(F32)
        hand[0, k] = (got[k, 2].astype(F32) + branch).astype(BF16)
        hp_copy(k).start()

    half[...] = jnp.dot(amat[core], hand[0].reshape(SLOTS, 128), preferred_element_type=F32)

    a_swap.wait_recv()
    arrived(hpar, swap_r.at[2])

    theirs = hpar[...].reshape(SLOTS, 128)

    def p1y_copy(d, i, first, count):
        to = lax.rem(y + d, NY)
        zs = pl.ds(first, count)
        return remote(
            s1p.at[zs, to], r1y.at[d - 1, zs], p1y_s.at[0], p1y_r.at[i], (rank_of(to, zlo), mp)
        )

    def p1z_copy(to):
        return remote(s1p.at[to], r1z.at[from_z(to)], p_s.at[0], p_r.at[0], (rank_of(y, to), mp))

    def p2z_copy(to):
        return remote(s2z.at[to], r2z.at[from_z(to)], p_s.at[1], p_r.at[1], (rank_of(y, to), mp))

    def p2y_copy(d):
        to = lax.rem(y + d, NY)
        return remote(s2y.at[to], r2y.at[d - 1], p_s.at[2], p_r.at[2], (rank_of(to, zlo), mp))

    def block_rows(z):
        rows = pl.ds(pl.multiple_of(z * NY * BLK, 16), NY * BLK)
        res = half[rows, :] + jnp.dot(apar[rows, :], theirs, preferred_element_type=F32)
        s1p[z] = res.astype(BF16).reshape(NY, BLK, 128)

    def kv_sum():
        total = s1k[y].astype(F32)
        arrived(r1k, k_r.at[0])
        for d in range(1, NY):
            total = total + r1k[d - 1].astype(F32)
        s2k[...] = total.astype(BF16)
        for to in far:
            kz_copy(to).start()

    def send_y(i, first, count):
        for z in range(first, first + count):
            block_rows(z)
        for d in FAR_Y:
            p1y_copy(d, i, first, count).start()

    def send_z(z):
        block_rows(z)

        @pl.when(zlo != z)
        def _():
            p1z_copy(z).start()

    def sum_y(i, first, count):
        total = s1p[first : first + count, y].astype(F32)
        arrived(r1y.at[:, pl.ds(first, count)], p1y_r.at[i])
        for d in range(1, NY):
            total = total + r1y[d - 1, first : first + count].astype(F32)
        s2z[first : first + count] = total.astype(BF16)
        for z in range(first, first + count):
            @pl.when(zlo != z)
            def _():
                p2z_copy(z).start()

    def one_of(zs):
        hit = zlo == zs[0]
        for z in zs[1:]:
            hit = hit | (zlo == z)
        return hit

    def sum_z(zs):
        @pl.when(one_of(zs))
        def _():
            total = s1p[zlo].astype(F32)
            arrived(r1z, p_r.at[0])
            for d in range(1, NZ):
                total = total + r1z[d - 1].astype(F32)
            s2y[...] = total.astype(BF16)
            for d in FAR_Y:
                p2y_copy(d).start()

    def follow(c, steps):
        groups, zs = Y_GROUPS[c], Z_FIRST[c]

        @pl.when(core == c)
        def _():
            for kind, i in steps:
                if kind == "kv":
                    kv_sum()
                elif kind == "sum_y":
                    sum_y(i, *groups[i])
                elif kind == "sum_z":
                    sum_z(zs)
                elif kind == "y":
                    send_y(i, *groups[i])
                else:
                    send_z(i)

    for c in range(NCORE):
        follow(c, SENDS[c])
    for c in range(NCORE):
        follow(c, SUMS[c])

    total = s2k[zlo].astype(F32)
    arrived(r2k, k_r.at[1])
    for d in range(1, NZ):
        total = total + r2k[d - 1].astype(F32)
    keyv[...] = total[:OWN, :64]
    valv[...] = total[:OWN, 64:]

    a_swap.wait_send()
    arrived(hpar, swap_s.at[2])
    arrived(xr, x_s.at[0])
    arrived(got, got_s.at[0])
    arrived(r1k, k_s.at[0])
    arrived(r2k, k_s.at[1])

    for c in range(NCORE):
        @pl.when(core == c)
        def _():
            zs = Z_FIRST[c]
            arrived(r1y.at[:, pl.ds(0, NZ - len(zs))], p1y_s.at[0])
            if not zs:
                arrived(r2z, p_s.at[1])
                return
            mine = one_of(zs)

            @pl.when(mine)
            def _():
                if len(zs) > 1:
                    arrived(r1z.at[0 : len(zs) - 1], p_s.at[0])
                if len(zs) < NZ:
                    arrived(s2z.at[0 : NZ - len(zs)], p_s.at[1])

            @pl.when(jnp.logical_not(mine))
            def _():
                arrived(r1z.at[0 : len(zs)], p_s.at[0])
                if len(zs) < NZ - 1:
                    arrived(s2z.at[0 : NZ - len(zs) - 1], p_s.at[1])

    z_first = jnp.bool_(False)
    for c in range(NCORE):
        if Z_FIRST[c]:
            z_first = z_first | ((core == c) & one_of(Z_FIRST[c]))

    @pl.when(z_first)
    def _():
        total = s2y[y].astype(F32)
        arrived(r2y, p_r.at[2])
        for d in range(1, NY):
            total = total + r2y[d - 1].astype(F32)
        projv[...] = total[:OWN, :]
        arrived(r2y, p_s.at[2])

    @pl.when(jnp.logical_not(z_first))
    def _():
        total = s2z[zlo].astype(F32)
        arrived(r2z, p_r.at[1])
        for d in range(1, NZ):
            total = total + r2z[d - 1].astype(F32)
        projv[...] = total[:OWN, :]


def writer(key_i, val_i, proj_i, hand_i, key_o, val_o, proj_o, hand_o, sem):
    pairs = ((key_i, key_o), (val_i, val_o), (proj_i, proj_o), (hand_i, hand_o))
    copies = [pltpu.make_async_copy(s, d, sem.at[i]) for i, (s, d) in enumerate(pairs)]
    for c in copies:
        c.start()
    for c in copies:
        c.wait()


def per_device(
    hidden_rows, key_grad, value_grad, visual_rows, visual_cotangent, norm_gain, norm_bias,
    fc1_weight, fc1_bias, fc2_weight, fc2_bias, layer_scale, token_counts, dest_offsets,
):
    anyspec = pl.BlockSpec(memory_space=pl.ANY)
    vmem = pl.BlockSpec(memory_space=pltpu.VMEM)
    dma = pltpu.SemaphoreType.DMA
    V = pltpu.VMEM
    S = pltpu.SMEM
    scratch = [
        V((512, WIDE), BF16), V((128, 512), BF16), V((256, 1024), BF16), V((4, 64, WIDE), BF16), V((4, 1024), F32),
        V((1024, 512), BF16), V((1, 512), F32), V((512, 1024), BF16), S((2, IMAGES), jnp.int32),
        V((256, 1024), BF16), V((256, 1024), BF16), V((256, 512), BF16), V((NHALF, 256, 512), F32),
        V((NHALF, NX, SPREAD, CAP, 128), BF16), V((NHALF, SPREAD, NX - 1, CAP, 128), BF16),
        V((SPREAD, CAP, 128), BF16), V((NHALF, SPREAD, CAP, 128), BF16), V((SPREAD, 3, CAP, 128), BF16),
        V((SPREAD, CAP, 128), BF16),
        V((WIDE + 80, 128), F32), V((NCORE, NY, NZ, BLK, 128), F32), V((NY, NZ, BLK, 128), F32),
        V((WIDE + 80, 256), F32), V((NCORE, N_CHIP * BLK, 256), BF16), V((N_CHIP * BLK, 256), BF16),
        V((N_CHIP * BLK, 128), F32),
        V((NY, NZ, BLK, 128), BF16), V((NY - 1, NZ, BLK, 128), BF16),
        V((NZ, BLK, 128), BF16), V((NZ - 1, BLK, 128), BF16),
        V((NZ, NY, BLK, 128), BF16), V((NY - 1, NZ, BLK, 128), BF16), V((NZ - 1, NY, BLK, 128), BF16),
        V((NZ, BLK, 128), BF16), V((NY, BLK, 128), BF16), V((NZ - 1, BLK, 128), BF16), V((NY - 1, BLK, 128), BF16),
        dma((9,)), dma((3,)), dma((3,)), dma((1,)), dma((SPREAD + 1,)), dma((1,)), dma((SPREAD,)),
        dma((2,)), dma((2,)), dma((1,)), dma((N_GROUPS,)), dma((3,)), dma((3,)),
        pltpu.SemaphoreType.REGULAR((3,)),
    ]
    shapes = (
        jax.ShapeDtypeStruct((OWN, 64), F32),
        jax.ShapeDtypeStruct((OWN, 64), F32),
        jax.ShapeDtypeStruct((OWN, 128), F32),
        jax.ShapeDtypeStruct((1, SPREAD, CAP, 128), BF16),
    )
    held = (V((OWN, 64), F32), V((OWN, 64), F32), V((OWN, 128), F32), V((1, SPREAD, CAP, 128), BF16))
    results = pl.pallas_call(
        kernel,
        out_shape=held,
        in_specs=[anyspec] * 14,
        out_specs=[vmem] * 4,
        scratch_shapes=scratch,
        compiler_params=pltpu.CompilerParams(
            collective_id=0, has_side_effects=True, vmem_limit_bytes=60 * 1024 * 1024
        ),
        name="bucket",
    )(
        hidden_rows, key_grad.T, value_grad.T, visual_rows, visual_cotangent,
        norm_gain.reshape(1, -1), norm_bias.reshape(1, -1), fc1_weight, fc1_bias.reshape(1, -1),
        fc2_weight, fc2_bias.reshape(1, -1), layer_scale.reshape(1, -1), token_counts, dest_offsets,
    )
    return pl.pallas_call(
        writer,
        out_shape=shapes,
        in_specs=[vmem] * 4,
        out_specs=[anyspec] * 4,
        scratch_shapes=[dma((4,))],
        name="writer",
    )(*[pltpu.with_memory_space_constraint(r, pltpu.VMEM) for r in results])


def solution(mesh):
    placed = (
        P("dp", None), P("dp", "mp"), P("dp", "mp"), P("dp", None), P("dp", None, None, None),
        P(), P(), P(None, "mp"), P("mp"), P("mp", None), P(), P(), P("dp", None), P("dp", None),
    )
    return jax.shard_map(
        per_device,
        mesh=mesh,
        in_specs=placed,
        out_specs=(P("dp", "mp"), P("dp", "mp"), P("dp", "mp"), P("dp", None, None, "mp")),
        check_vma=False,
    )
```
